32 devices in a mesh: tgt: 8 (over z, y), src: 2 (over x), grp: 2 (over core).
Axes of the slice: x: 2, y: 2, z: 4, core: 2. Of those that a mesh axis runs over, the one named last changes fastest.
Arguments:
- positions: float32 [3, 2048], P(None, ('tgt', 'src', 'grp')), may hold values from 0 to 1
- strengths: float32 [3, 2048], P(None, ('tgt', 'src', 'grp')), may hold values from -0.02 to 0.02
- live_counts: int32 [32], P(('tgt', 'src', 'grp')), may hold values from 1 to 64, 1280 in all
- vorticity: float32 [3, 96, 96, 256], P(None, 'tgt', ('src', 'grp')), may hold values from -6 to 6
- diffusivity: float32 [96, 96, 256], P('tgt', ('src', 'grp')), may hold values from 0.02 to 0.15
- seed_counts: int32 [96, 96, 256], P('tgt', ('src', 'grp')), may hold values from 0 to 7
Outputs:
- vorticity_next: float32 [3, 96, 96, 256], P(None, 'tgt', ('src', 'grp'))
- particle_rates: float32 [6, 2048], P(None, ('tgt', 'src', 'grp'))
- blob_velocity: float32 [3, 4096], P(None, ('tgt', 'src', 'grp'))
The draws below stay inside these ranges and needn't reach their ends.
Inputs may be any that keep to these rules, and one draw needn't show every extreme that they name: `live_counts`: the values sum to 32 * 64 * 5 // 8.
All inputs are finite; a program needn't handle non-finite values.
Results may differ from the reference program's by a relative error of at most 0.000095.
Values sent between devices are 32-bit elements; how exact they have to be, the bound alone decides.
No kernel may reach another device: no remote copies, remote signals or barrier semaphores. Data moves between devices by JAX's collectives and lax.ppermute only.
A program may use at most 64 MiB of HBM per device.

```python
import math
import jax
import jax.numpy as jnp
import numpy as np
from jax import lax

P_DEV = 64
CX = 12
CY = 24
GZ = 256
BZ = 2
B_DEV = 128
E_DEV = 192
NP = 2048
GX = 96
GY = 96
N_TGT = 8
DEVICES = 32


def with_ends(entries, key, low, top_value):
    longest = entries.shape.index(max(entries.shape))
    spots = []
    for shift in (0, 1):
        where = [jax.random.randint(jax.random.fold_in(key, axis), (), 0, length) for axis, length in enumerate(entries.shape)]
        where[longest] = (where[longest] + shift) % entries.shape[longest]
        spots.append(tuple(where))
    return entries.at[spots[0]].set(low).at[spots[1]].set(top_value)


def level_of(own_key, shape, pieces, smallest, high):
    level, own = 1.0, jax.random.fold_in(own_key, 6)
    for position, shards_of in pieces:
        draws = jnp.exp(jax.random.uniform(jax.random.fold_in(own, position), (shards_of,), jnp.float32, smallest / len(pieces), high / len(pieces)))
        level = level * jnp.repeat(draws, shape[position] // shards_of).reshape([-1 if axis == position else 1 for axis in range(len(shape))])
    return level


def split_up(amount, total, limit, lean):
    weights = [(1 << 20) // math.isqrt(rank ** lean) + 1 for rank in range(2, amount + 1)]
    rest, holding = total - limit - (amount - 1), [1] * (amount - 1)
    while rest > 0:
        candidates = [i for i in range(amount - 1) if holding[i] < limit]
        pool, left = sum([weights[i] for i in candidates]), rest
        for i in candidates:
            addition = min(limit - holding[i], max(1, left * weights[i] // pool), rest)
            holding[i] = holding[i] + addition
            rest = rest - addition
    return np.array([limit] + holding)


def ragged_sizes(rng, number_of, total, reach, lean):
    if number_of == 2:
        one = jax.random.randint(rng, (), max(1, total - reach), min(reach, total - 1) + 1)
        return jnp.stack([one, total - one])
    lengths = jnp.asarray(split_up(number_of, total, reach, lean), jnp.int32)
    couples = (number_of - 1) // 2
    giver, sink = lengths[1:1 + 2 * couples:2], lengths[2:2 + 2 * couples:2]
    room = jnp.minimum(giver - 1, reach - sink)
    shifted = jax.random.randint(jax.random.fold_in(rng, 1), (couples,), 0, 1 << 20) % (room + 1)
    lengths = lengths.at[1:1 + 2 * couples:2].set(giver - shifted).at[2:2 + 2 * couples:2].set(sink + shifted)
    return lengths[jax.random.permutation(jax.random.fold_in(rng, 2), number_of)]


def gaussian(key, shape, width, most, shards=(), held_as=jnp.bfloat16):
    drawn = jax.random.normal(key, shape, jnp.float32) * width
    if len(shards) > 0:
        drawn = level_of(key, shape, shards, -0.22, 0.18) * drawn
    return jnp.clip(drawn, min=-most, max=most).astype(held_as)


def setup_inputs(seed: int = 0) -> dict:
    key_of = jax.random.split(jax.random.key(seed), 7)
    return {
        "positions": jnp.clip(1.0 * jax.random.uniform(key_of[0], (3, NP), jnp.float32) ** level_of(key_of[0], (3, NP), ((1, 32),), -0.2, 0.2), 0.0, 1.0),
        "strengths": gaussian(key_of[1], (3, NP), 0.003, 0.02, ((1, 32),), jnp.float32),
        "live_counts": ragged_sizes(key_of[2], DEVICES, DEVICES * P_DEV * 5 // 8, P_DEV, 2).astype(jnp.int32),
        "vorticity": gaussian(key_of[3], (3, GX, GY, GZ), 1.0, 6.0, ((1, 8), (2, 4)), jnp.float32),
        "diffusivity": jnp.clip(0.02 + 0.13000001 * jax.random.uniform(key_of[4], (GX, GY, GZ), jnp.float32) ** level_of(key_of[4], (GX, GY, GZ), ((0, 8), (1, 4)), -0.2, 0.2), 0.02, 0.15),
        "seed_counts": with_ends(jax.random.randint(key_of[5], (GX, GY, GZ), 0, 8), jax.random.fold_in(key_of[5], 1), 0, 7).astype(jnp.int32),
    }


sigma_sq = 0.0004
kernel_scale = 0.25 / 3.141592653589793
seed_weight = 0.0001

def pair_rates(targets, sources):
    sep_x = targets[0][:, None] - sources[0][None, :]
    sep_y = targets[1][:, None] - sources[1][None, :]
    sep_z = targets[2][:, None] - sources[2][None, :]
    squared = sep_x * sep_x + sep_y * sep_y + sep_z * sep_z + sigma_sq
    inverse = lax.rsqrt(squared)
    kernel = inverse * inverse * inverse
    kernel_five = kernel * inverse * inverse
    cross_x = sep_y * sources[5][None, :] - sep_z * sources[4][None, :]
    cross_y = sep_z * sources[3][None, :] - sep_x * sources[5][None, :]
    cross_z = sep_x * sources[4][None, :] - sep_y * sources[3][None, :]
    projected = targets[3][:, None] * sep_x + targets[4][:, None] * sep_y + targets[5][:, None] * sep_z
    weighted = 3.0 * kernel_five * projected
    velocity = jnp.stack([lax.optimization_barrier(jnp.sum(kernel * cross_x, axis=1)), lax.optimization_barrier(jnp.sum(kernel * cross_y, axis=1)), lax.optimization_barrier(jnp.sum(kernel * cross_z, axis=1))])
    pulled_x = lax.optimization_barrier(jnp.sum(kernel * sources[3][None, :], axis=1))
    pulled_y = lax.optimization_barrier(jnp.sum(kernel * sources[4][None, :], axis=1))
    pulled_z = lax.optimization_barrier(jnp.sum(kernel * sources[5][None, :], axis=1))
    first_term = jnp.stack([targets[4] * pulled_z - targets[5] * pulled_y, targets[5] * pulled_x - targets[3] * pulled_z, targets[3] * pulled_y - targets[4] * pulled_x])
    second_term = jnp.stack([lax.optimization_barrier(jnp.sum(weighted * cross_x, axis=1)), lax.optimization_barrier(jnp.sum(weighted * cross_y, axis=1)), lax.optimization_barrier(jnp.sum(weighted * cross_z, axis=1))])
    return (-kernel_scale * velocity, -kernel_scale * (first_term - second_term))

def laplace(padded):
    centre = padded[:, 1:-1, 1:-1, 1:-1]
    beside_all = padded[:, 2:, 1:-1, 1:-1] + padded[:, :-2, 1:-1, 1:-1]
    beside_all = beside_all + padded[:, 1:-1, 2:, 1:-1] + padded[:, 1:-1, :-2, 1:-1]
    beside_all = beside_all + padded[:, 1:-1, 1:-1, 2:] + padded[:, 1:-1, 1:-1, :-2]
    return beside_all - 6.0 * centre

def reference(positions, strengths, live_counts, vorticity, diffusivity, seed_counts):
    padded = jnp.pad(vorticity, ((0, 0), (1, 1), (1, 1), (1, 1)))
    vorticity_next = vorticity + diffusivity[None] * laplace(padded)
    counts = seed_counts.astype(jnp.float32)
    grid_y = vorticity.shape[2]
    y_slabs = grid_y // CY
    z_blocks = GZ // BZ
    blob_strength = seed_weight * lax.optimization_barrier(jnp.sum((vorticity_next * counts[None]).reshape(3, N_TGT, CX, y_slabs, CY, z_blocks, BZ), axis=(2, 4, 6)))
    blob_strength = blob_strength.reshape(3, DEVICES, B_DEV)
    weights = (counts + 1.0).reshape(N_TGT, CX, y_slabs, CY, z_blocks, BZ)
    totals = lax.optimization_barrier(jnp.sum(weights, axis=(1, 3, 5)))
    x_centres = ((jnp.arange(N_TGT * CX, dtype=jnp.float32) + 0.5) / GZ).reshape(N_TGT, CX)
    y_centres = ((jnp.arange(grid_y, dtype=jnp.float32) + 0.5) / GZ).reshape(y_slabs, CY)
    z_centres = ((jnp.arange(GZ, dtype=jnp.float32) + 0.5) / GZ).reshape(z_blocks, BZ)
    blob_x = lax.optimization_barrier(jnp.sum(lax.optimization_barrier(jnp.sum(weights, axis=(3, 5))) * x_centres[:, :, None, None], axis=1))
    blob_y = lax.optimization_barrier(jnp.sum(lax.optimization_barrier(jnp.sum(weights, axis=(1, 5))) * y_centres[None, :, :, None], axis=2))
    blob_z = lax.optimization_barrier(jnp.sum(lax.optimization_barrier(jnp.sum(weights, axis=(1, 3))) * z_centres[None, None], axis=3))
    blob_position = (jnp.stack([blob_x, blob_y, blob_z]) / totals[None]).reshape(3, DEVICES, B_DEV)
    live_mask = (jnp.arange(P_DEV, dtype=jnp.int32)[None, :] < live_counts[:, None]).astype(jnp.float32)
    particle_pos = positions.reshape(3, DEVICES, P_DEV)
    particle_str = strengths.reshape(3, DEVICES, P_DEV) * live_mask[None]
    elements = jnp.concatenate([jnp.concatenate([particle_pos, blob_position], axis=2), jnp.concatenate([particle_str, blob_strength], axis=2)], axis=0)
    sources = elements.reshape(6, DEVICES * E_DEV)

    def per_device(targets):
        velocity, stretch = pair_rates(targets, sources)
        return jnp.concatenate([velocity, stretch], axis=0)
    all_rates = lax.map(per_device, jnp.moveaxis(elements, 1, 0))
    particle_rates = jnp.moveaxis(all_rates[:, :, :P_DEV] * live_mask[:, None, :], 0, 1).reshape(6, DEVICES * P_DEV)
    blob_velocity = jnp.moveaxis(all_rates[:, :3, P_DEV:], 0, 1).reshape(3, DEVICES * B_DEV)
    return (vorticity_next, particle_rates, blob_velocity)
```

```python
import functools
import jax
import jax.numpy as jnp
from jax import lax
from jax.experimental import pallas as pl
from jax.experimental.pallas import tpu as pltpu
from jax.sharding import PartitionSpec as P

BZ = 2
LANES = 128
GROUPS = 9

sigma_sq = 0.0004
kernel_scale = 0.25 / 3.141592653589793
seed_weight = 0.0001


VMEM = pl.BlockSpec(memory_space=pltpu.VMEM)
SMEM = pl.BlockSpec(memory_space=pltpu.SMEM)


def split3(value):
    high = value.astype(jnp.bfloat16)
    rest = value - high.astype(jnp.float32)
    middle = rest.astype(jnp.bfloat16)
    low = (rest - middle.astype(jnp.float32)).astype(jnp.bfloat16)
    return high, middle, low


def pair_lanes(rows):
    length = rows.shape[1]
    cell = lax.broadcasted_iota(jnp.int32, (length, length // BZ), 0)
    blob = lax.broadcasted_iota(jnp.int32, (length, length // BZ), 1)
    chosen = jnp.where((cell >= blob * BZ) & (cell < blob * BZ + BZ), 1.0, 0.0).astype(jnp.bfloat16)
    total = None
    for part in split3(rows):
        product = jnp.dot(part, chosen, preferred_element_type=jnp.float32)
        total = product if total is None else total + product
    return total


def shifted_rows(value, step):
    rows = lax.broadcasted_iota(jnp.int32, value.shape, 0)
    count = value.shape[0]
    if step == 1:
        return jnp.where(rows == 0, 0.0, pltpu.roll(value, 1, 0))
    return jnp.where(rows == count - 1, 0.0, pltpu.roll(value, count - 1, 0))


def shifted_lanes(value, step):
    lanes = lax.broadcasted_iota(jnp.int32, value.shape, 1)
    count = value.shape[1]
    if step == 1:
        return jnp.where(lanes == 0, 0.0, pltpu.roll(value, 1, 1))
    return jnp.where(lanes == count - 1, 0.0, pltpu.roll(value, count - 1, 1))


def local_kernel(place_ref, v_ref, d_ref, c_ref, sums_ref, wx_ref, wy_ref, pos_ref):
    _, cells_x, cells_y, cells_z = v_ref.shape
    w = []
    c = []
    for x in range(cells_x):
        counts = c_ref[x].astype(jnp.float32)
        c.append(counts)
        w.append(counts * d_ref[x])
    wx_ref[0] = w[0]
    wx_ref[1] = w[cells_x - 1]
    for x in range(cells_x):
        wy_ref[0, x : x + 1, :] = w[x][0:1, :]
        wy_ref[1, x : x + 1, :] = w[x][cells_y - 1 : cells_y, :]
    zero = jnp.zeros((cells_y, cells_z), jnp.float32)
    at = [zero] * 3
    after = [zero] * 3
    before = [zero] * 3
    plain = zero
    moment = zero
    for x in range(cells_x):
        beside = shifted_rows(w[x], 1) + shifted_rows(w[x], -1)
        if x > 0:
            beside = beside + w[x - 1]
        if x < cells_x - 1:
            beside = beside + w[x + 1]
        here = c[x] + (beside - 6.0 * w[x])
        up = shifted_lanes(w[x], 1)
        down = shifted_lanes(w[x], -1)
        for k in range(3):
            v = v_ref[k, x]
            at[k] = at[k] + here * v
            after[k] = after[k] + up * v
            before[k] = before[k] + down * v
        plain = plain + (c[x] + 1.0)
        moment = moment + (c[x] + 1.0) * (x + 0.5)
    rows = []
    for k in range(3):
        total = (
            jnp.sum(at[k], axis=0, keepdims=True)
            + shifted_lanes(jnp.sum(after[k], axis=0, keepdims=True), -1)
            + shifted_lanes(jnp.sum(before[k], axis=0, keepdims=True), 1)
        )
        rows.append(total)
    sums_ref[0:3, :] = jnp.concatenate(rows, axis=0)
    sums_ref[3:8, :] = jnp.zeros((5, cells_z), jnp.float32)
    y_centre = lax.broadcasted_iota(jnp.int32, (cells_y, cells_z), 0).astype(jnp.float32) + 0.5
    z_centre = lax.broadcasted_iota(jnp.int32, (1, cells_z), 1).astype(jnp.float32) + 0.5
    weight = jnp.sum(plain, axis=0, keepdims=True)
    moments = jnp.concatenate(
        [
            weight,
            jnp.sum(moment, axis=0, keepdims=True),
            jnp.sum(plain * y_centre, axis=0, keepdims=True),
            weight * z_centre,
            jnp.zeros((4, cells_z), jnp.float32),
        ],
        axis=0,
    )
    blobs = pair_lanes(moments)
    inverse = 1.0 / blobs[0:1]
    x_anchor = place_ref[0].astype(jnp.float32)
    y_anchor = place_ref[1].astype(jnp.float32)
    pos_ref[0:1, :] = (blobs[1:2] * inverse + x_anchor) / cells_z
    pos_ref[1:2, :] = (blobs[2:3] * inverse + y_anchor) / cells_z
    pos_ref[2:3, :] = (blobs[3:4] * inverse) / cells_z


def block_kernel(place_ref, sums_ref, wx_ref, wy_ref, pos_ref, part_ref, xa_ref, xb_ref, ya_ref, yb_ref, out_ref):
    x_even = place_ref[2] == 0
    y_even = place_ref[3] == 0
    total = sums_ref[...]
    rows = []
    for k in range(3):
        first = jnp.where(x_even, xb_ref[k], xa_ref[k])
        last = jnp.where(x_even, xa_ref[k], xb_ref[k])
        row = jnp.sum(wx_ref[0] * first + wx_ref[1] * last, axis=0, keepdims=True)
        first = jnp.where(y_even, yb_ref[k], ya_ref[k])
        last = jnp.where(y_even, ya_ref[k], yb_ref[k])
        row = row + jnp.sum(wy_ref[0] * first + wy_ref[1] * last, axis=0, keepdims=True)
        rows.append(row)
    total = total + jnp.concatenate(rows + [jnp.zeros((5, total.shape[1]), jnp.float32)], axis=0)
    strength = seed_weight * pair_lanes(total)
    block = jnp.concatenate([pos_ref[...], strength[0:3], part_ref[...]], axis=0)
    devices = out_ref.shape[0] // GROUPS
    for device in range(devices):
        out_ref[device * GROUPS : (device + 1) * GROUPS, :] = block


def grid_kernel(place_ref, v_ref, d_ref, xa_ref, xb_ref, ya_ref, yb_ref, out_ref):
    _, cells_x, cells_y, cells_z = v_ref.shape
    x_even = place_ref[2] == 0
    y_even = place_ref[3] == 0
    rows = lax.broadcasted_iota(jnp.int32, (cells_y, cells_z), 0)
    for k in range(3):
        before = jnp.where(x_even, xb_ref[k], xa_ref[k])
        beyond = jnp.where(x_even, xa_ref[k], xb_ref[k])
        first = jnp.where(y_even, yb_ref[k], ya_ref[k])
        last = jnp.where(y_even, ya_ref[k], yb_ref[k])
        for x in range(cells_x):
            v = v_ref[k, x]
            low = before if x == 0 else v_ref[k, x - 1]
            high = beyond if x == cells_x - 1 else v_ref[k, x + 1]
            left = jnp.where(rows == 0, first[x : x + 1], pltpu.roll(v, 1, 0))
            right = jnp.where(rows == cells_y - 1, last[x : x + 1], pltpu.roll(v, cells_y - 1, 0))
            beside = (high + low) + (right + left) + (shifted_lanes(v, -1) + shifted_lanes(v, 1))
            out_ref[k, x] = v + d_ref[x] * (beside - 6.0 * v)


def pair_kernel(centre_ref, live_ref, all_ref, own_ref, rates_ref, blob_ref, source_ref, feature_ref, column_ref, sum_ref, pull_ref, turn_ref):
    devices = all_ref.shape[0] // GROUPS
    half = LANES // 2
    tiles = devices + devices // 2
    lane = lax.broadcasted_iota(jnp.int32, (devices, LANES), 1)
    centre = [centre_ref[0], centre_ref[1], centre_ref[2]]

    def group(index):
        return all_ref[pl.ds(index, devices, stride=GROUPS), :]

    blobs = [group(k) for k in range(6)]
    particles = []
    for k in range(3):
        both = group(6 + k)
        turned = pltpu.roll(both, half, 1)
        particles.append(jnp.where(lane < half, both, pltpu.roll(turned, devices - 1, 0)))
        particles.append(jnp.where(lane < half, turned, pltpu.roll(both, devices - 1, 0)))

    def put(ref, index, stride, blob_rows, particle_rows):
        ref[pl.ds(index, devices, stride=stride), :] = blob_rows
        turn_ref[...] = particle_rows
        ref[pl.ds(devices * stride + index, devices // 2, stride=stride), :] = turn_ref[pl.ds(0, devices // 2, stride=2), :]

    for k in range(3):
        put(source_ref, k, 8, blobs[k], particles[k])

    def features(parts):
        place = [parts[k] - centre[k] for k in range(3)]
        a = parts[3:]
        return a + [
            place[1] * a[2] - place[2] * a[1],
            place[2] * a[0] - place[0] * a[2],
            place[0] * a[1] - place[1] * a[0],
        ]

    feature_ref[...] = jnp.zeros_like(feature_ref)
    blob_features = features(blobs)
    particle_features = features(particles)
    for k in range(6):
        blob_parts = split3(blob_features[k])
        particle_parts = split3(particle_features[k])
        for j in range(3):
            put(feature_ref, 8 * j + k, 32, blob_parts[j].astype(jnp.float32), particle_parts[j].astype(jnp.float32))

    own = own_ref[0:GROUPS, :]
    target_rows = []
    for k in range(3):
        row = own[6 + k : 7 + k]
        target_rows.append(row)
        target_rows.append(pltpu.roll(row, half, 1))
    zeros = jnp.zeros((1, LANES), jnp.float32)
    wide = [jnp.concatenate([own[k : k + 1], target_rows[k]], axis=1) for k in range(3)]
    wide = wide + [jnp.concatenate([zeros, target_rows[k]], axis=1) for k in range(3, 6)]
    table = jnp.concatenate(wide + [jnp.zeros((LANES - 6, 2 * LANES), jnp.float32)], axis=0)
    columns = jnp.transpose(table)
    targets = LANES + half
    for k in range(6):
        column_ref[k] = jnp.broadcast_to(columns[0:targets, k : k + 1], (targets, LANES))

    sum_ref[...] = jnp.zeros_like(sum_ref)
    pull_ref[...] = jnp.zeros_like(pull_ref)
    block = 64
    contract = (((1,), (1,)), ((), ()))

    def step(chunk, _):
        base = chunk * 2
        feature = feature_ref[pl.ds(pl.multiple_of(base * 32, 64), 64), :].astype(jnp.bfloat16)
        feature = jnp.concatenate([feature[0:32], feature[32:64]], axis=1)
        source = source_ref[pl.ds(pl.multiple_of(base * 8, 16), 16), :]
        for t in range(0, targets, block):
            highs, lows, pull_highs, pull_lows = [], [], [], []
            for j in range(2):
                sep = [column_ref[k, t : t + block, :] - source[8 * j + k : 8 * j + k + 1] for k in range(3)]
                squared = sep[0] * sep[0] + sep[1] * sep[1] + (sep[2] * sep[2] + sigma_sq)
                inverse = lax.rsqrt(squared)
                square = inverse * inverse
                kernel = square * inverse
                high = kernel.astype(jnp.bfloat16)
                highs.append(high)
                lows.append((kernel - high.astype(jnp.float32)).astype(jnp.bfloat16))
                if t >= LANES:
                    along = column_ref[3, t : t + block, :] * sep[0] + column_ref[4, t : t + block, :] * sep[1] + column_ref[5, t : t + block, :] * sep[2]
                    weighted = (kernel * square) * along
                    high = weighted.astype(jnp.bfloat16)
                    pull_highs.append(high)
                    pull_lows.append((weighted - high.astype(jnp.float32)).astype(jnp.bfloat16))
            total = lax.dot_general(jnp.concatenate(highs, axis=1), feature, contract, preferred_element_type=jnp.float32)
            total = total + lax.dot_general(jnp.concatenate(lows, axis=1), feature, contract, preferred_element_type=jnp.float32)
            sum_ref[t : t + block, 0:32] = sum_ref[t : t + block, 0:32] + total
            if t >= LANES:
                total = lax.dot_general(jnp.concatenate(pull_highs, axis=1), feature, contract, preferred_element_type=jnp.float32)
                total = total + lax.dot_general(jnp.concatenate(pull_lows, axis=1), feature, contract, preferred_element_type=jnp.float32)
                pull_ref[0:block, 0:32] = pull_ref[0:block, 0:32] + total
        return 0

    lax.fori_loop(0, tiles // 2, step, 0)

    def combined(table):
        turned = jnp.transpose(table)
        return turned[0:8] + turned[8:16] + turned[16:24]

    found = combined(sum_ref[...])
    pulled = combined(pull_ref[...])

    def crossed(place, rows):
        return [
            place[1] * rows[2:3] - place[2] * rows[1:2] - rows[3:4],
            place[2] * rows[0:1] - place[0] * rows[2:3] - rows[4:5],
            place[0] * rows[1:2] - place[1] * rows[0:1] - rows[5:6],
        ]

    place = [wide[k] - centre[k] for k in range(3)]
    velocity = [-kernel_scale * row for row in crossed(place, found)]
    a = target_rows[3:]
    own_place = [target_rows[k] - centre[k] for k in range(3)]
    second = crossed(own_place, pulled)
    near = found[:, LANES:]
    first = [
        a[1] * near[2:3] - a[2] * near[1:2],
        a[2] * near[0:1] - a[0] * near[2:3],
        a[0] * near[1:2] - a[1] * near[0:1],
    ]
    stretch = [-kernel_scale * (first[k] - 3.0 * second[k]) for k in range(3)]
    alive = (lax.broadcasted_iota(jnp.int32, (1, LANES), 1) < live_ref[0]).astype(jnp.float32)
    for k in range(3):
        blob_ref[k : k + 1, :] = velocity[k][:, 0:LANES]
        rates_ref[k : k + 1, :] = (velocity[k][:, LANES:] * alive)[:, 0:half]
        rates_ref[3 + k : 4 + k, :] = (stretch[k] * alive)[:, 0:half]


def partners(count, start):
    pairs = [(i, i + 1) for i in range(start, count - 1, 2)]
    return pairs + [(j, i) for i, j in pairs]


def per_device(positions, strengths, live_counts, vorticity, diffusivity, seed_counts):
    _, cells_x, cells_y, cells_z = vorticity.shape
    slot_count = positions.shape[1]
    y_axes = ("src", "grp")
    everyone = ("tgt", "src", "grp")
    x_count, y_count = lax.axis_size("tgt"), lax.axis_size("src") * lax.axis_size("grp")
    devices = x_count * y_count
    x_index = lax.axis_index("tgt")
    y_index = lax.axis_index("src") * lax.axis_size("grp") + lax.axis_index("grp")
    x_even, y_even = x_index % 2 == 0, y_index % 2 == 0

    x_first, x_last = vorticity[:, 0], vorticity[:, cells_x - 1]
    y_first, y_last = vorticity[:, :, 0], vorticity[:, :, cells_y - 1]
    xa = lax.ppermute(jnp.where(x_even, x_last, x_first), "tgt", partners(x_count, 0))
    xb = lax.ppermute(jnp.where(x_even, x_first, x_last), "tgt", partners(x_count, 1))
    ya = lax.ppermute(jnp.where(y_even, y_last, y_first), y_axes, partners(y_count, 0))
    yb = lax.ppermute(jnp.where(y_even, y_first, y_last), y_axes, partners(y_count, 1))

    place = jnp.stack([x_index * cells_x, y_index * cells_y, x_index % 2, y_index % 2]).astype(jnp.int32)
    f32 = jnp.float32
    shape = jax.ShapeDtypeStruct
    sums, wx, wy, blob_position = pl.pallas_call(
        local_kernel,
        name="local",
        out_shape=(
            shape((8, cells_z), f32),
            shape((2, cells_y, cells_z), f32),
            shape((2, cells_x, cells_z), f32),
            shape((3, cells_z // BZ), f32),
        ),
        in_specs=[SMEM, VMEM, VMEM, VMEM],
        out_specs=[VMEM] * 4,
    )(place, vorticity, diffusivity, seed_counts)

    live_mask = (jnp.arange(slot_count, dtype=jnp.int32) < live_counts[0]).astype(f32)
    particle_rows = jnp.concatenate([positions, strengths * live_mask[None]], axis=0).reshape(3, 2 * slot_count)
    block = pl.pallas_call(
        block_kernel,
        name="block",
        out_shape=shape((devices * GROUPS, LANES), f32),
        in_specs=[SMEM] + [VMEM] * 9,
        out_specs=VMEM,
    )(place, sums, wx, wy, blob_position, particle_rows, xa, xb, ya, yb)
    everything = lax.all_to_all(block.reshape(-1), everyone, 0, 0, tiled=True).reshape(devices * GROUPS, LANES)

    vorticity_next = pl.pallas_call(
        grid_kernel,
        name="grid",
        out_shape=shape(vorticity.shape, f32),
        in_specs=[SMEM] + [VMEM] * 6,
        out_specs=VMEM,
    )(place, vorticity, diffusivity, xa, xb, ya, yb)

    centre = jnp.stack(
        [
            (x_index.astype(f32) + 0.5) * cells_x / cells_z,
            (y_index.astype(f32) + 0.5) * cells_y / cells_z,
            jnp.float32(0.5),
        ]
    )
    tiles = devices + devices // 2
    targets = LANES + slot_count
    particle_rates, blob_velocity = pl.pallas_call(
        pair_kernel,
        name="pairs",
        out_shape=(shape((6, slot_count), f32), shape((3, LANES), f32)),
        in_specs=[SMEM, SMEM, VMEM, VMEM],
        out_specs=[VMEM, VMEM],
        scratch_shapes=[
            pltpu.VMEM((tiles * 8, LANES), f32),
            pltpu.VMEM((tiles * 32, LANES), f32),
            pltpu.VMEM((6, targets, LANES), f32),
            pltpu.VMEM((2 * LANES, LANES), f32),
            pltpu.VMEM((LANES, LANES), f32),
            pltpu.VMEM((devices, LANES), f32),
        ],
    )(centre, live_counts, everything, block)
    return (vorticity_next, particle_rates, blob_velocity)


def solution(mesh):
    placed = (
        P(None, ("tgt", "src", "grp")),
        P(None, ("tgt", "src", "grp")),
        P(("tgt", "src", "grp")),
        P(None, "tgt", ("src", "grp"), None),
        P("tgt", ("src", "grp"), None),
        P("tgt", ("src", "grp"), None),
    )
    return jax.shard_map(
        per_device,
        mesh=mesh,
        in_specs=placed,
        out_specs=(
            P(None, "tgt", ("src", "grp"), None),
            P(None, ("tgt", "src", "grp")),
            P(None, ("tgt", "src", "grp")),
        ),
        check_vma=False,
    )
```

```python
import functools
import jax
import jax.numpy as jnp
from jax import lax
from jax.experimental import pallas as pl
from jax.experimental.pallas import tpu as pltpu
from jax.sharding import PartitionSpec as P

BZ = 2
LANES = 128
GROUPS = 9

sigma_sq = 0.0004
kernel_scale = 0.25 / 3.141592653589793
seed_weight = 0.0001


VMEM = pl.BlockSpec(memory_space=pltpu.VMEM)
SMEM = pl.BlockSpec(memory_space=pltpu.SMEM)


def split3(value):
    high = value.astype(jnp.bfloat16)
    rest = value - high.astype(jnp.float32)
    middle = rest.astype(jnp.bfloat16)
    low = (rest - middle.astype(jnp.float32)).astype(jnp.bfloat16)
    return high, middle, low


def pair_lanes(rows):
    length = rows.shape[1]
    cell = lax.broadcasted_iota(jnp.int32, (length, length // BZ), 0)
    blob = lax.broadcasted_iota(jnp.int32, (length, length // BZ), 1)
    chosen = jnp.where((cell >= blob * BZ) & (cell < blob * BZ + BZ), 1.0, 0.0).astype(jnp.bfloat16)
    total = None
    for part in split3(rows):
        product = jnp.dot(part, chosen, preferred_element_type=jnp.float32)
        total = product if total is None else total + product
    return total


def shifted_rows(value, step):
    rows = lax.broadcasted_iota(jnp.int32, value.shape, 0)
    count = value.shape[0]
    if step == 1:
        return jnp.where(rows == 0, 0.0, pltpu.roll(value, 1, 0))
    return jnp.where(rows == count - 1, 0.0, pltpu.roll(value, count - 1, 0))


def shifted_lanes(value, step):
    lanes = lax.broadcasted_iota(jnp.int32, value.shape, 1)
    count = value.shape[1]
    if step == 1:
        return jnp.where(lanes == 0, 0.0, pltpu.roll(value, 1, 1))
    return jnp.where(lanes == count - 1, 0.0, pltpu.roll(value, count - 1, 1))


def here():
    x_index = lax.axis_index("tgt")
    y_index = lax.axis_index("src") * lax.axis_size("grp") + lax.axis_index("grp")
    return x_index, y_index


def faces_kernel(v_ref, xa_ref, xb_ref, ya_ref, yb_ref, low_ref, high_ref, sems):
    _, cells_x, cells_y, _ = v_ref.shape
    x_index, y_index = here()
    x_even = lax.rem(x_index, 2) == 0
    y_even = lax.rem(y_index, 2) == 0
    top = (cells_y - 1) // 8 * 8
    last = cells_x - 1
    copies = [
        pltpu.make_async_copy(v_ref.at[:, jnp.where(x_even, 0, last)], xb_ref, sems.at[0]),
        pltpu.make_async_copy(v_ref.at[:, jnp.where(x_even, last, 0)], xa_ref, sems.at[1]),
        pltpu.make_async_copy(v_ref.at[:, :, 0:8], low_ref, sems.at[2]),
        pltpu.make_async_copy(v_ref.at[:, :, top : top + 8], high_ref, sems.at[3]),
    ]
    for copy in copies:
        copy.start()
    copies[2].wait()
    copies[3].wait()
    for k in range(3):
        first = low_ref[k, :, 0, :]
        final = high_ref[k, :, cells_y - 1 - top, :]
        ya_ref[k] = jnp.where(y_even, final, first)
        yb_ref[k] = jnp.where(y_even, first, final)
    copies[0].wait()
    copies[1].wait()


def local_kernel(live_ref, v_ref, d_ref, c_ref, position_ref, strength_ref, sums_ref, wx_ref, wy_ref, row_ref):
    _, cells_x, cells_y, cells_z = v_ref.shape
    slot_count = position_ref.shape[1]
    w = []
    c = []
    for x in range(cells_x):
        counts = c_ref[x].astype(jnp.float32)
        c.append(counts)
        w.append(counts * d_ref[x])
    wx_ref[0] = w[0]
    wx_ref[1] = w[cells_x - 1]
    for x in range(cells_x):
        wy_ref[0, x : x + 1, :] = w[x][0:1, :]
        wy_ref[1, x : x + 1, :] = w[x][cells_y - 1 : cells_y, :]
    zero = jnp.zeros((cells_y, cells_z), jnp.float32)
    at = [zero] * 3
    after = [zero] * 3
    before = [zero] * 3
    plain = zero
    moment = zero
    for x in range(cells_x):
        beside = shifted_rows(w[x], 1) + shifted_rows(w[x], -1)
        if x > 0:
            beside = beside + w[x - 1]
        if x < cells_x - 1:
            beside = beside + w[x + 1]
        around = c[x] + (beside - 6.0 * w[x])
        up = shifted_lanes(w[x], 1)
        down = shifted_lanes(w[x], -1)
        for k in range(3):
            v = v_ref[k, x]
            at[k] = at[k] + around * v
            after[k] = after[k] + up * v
            before[k] = before[k] + down * v
        plain = plain + (c[x] + 1.0)
        moment = moment + (c[x] + 1.0) * (x + 0.5)
    rows = []
    for k in range(3):
        total = (
            jnp.sum(at[k], axis=0, keepdims=True)
            + shifted_lanes(jnp.sum(after[k], axis=0, keepdims=True), -1)
            + shifted_lanes(jnp.sum(before[k], axis=0, keepdims=True), 1)
        )
        rows.append(total)
    sums_ref[0:3, :] = jnp.concatenate(rows, axis=0)
    sums_ref[3:8, :] = jnp.zeros((5, cells_z), jnp.float32)
    y_centre = lax.broadcasted_iota(jnp.int32, (cells_y, cells_z), 0).astype(jnp.float32) + 0.5
    z_centre = lax.broadcasted_iota(jnp.int32, (1, cells_z), 1).astype(jnp.float32) + 0.5
    weight = jnp.sum(plain, axis=0, keepdims=True)
    moments = jnp.concatenate(
        [
            weight,
            jnp.sum(moment, axis=0, keepdims=True),
            jnp.sum(plain * y_centre, axis=0, keepdims=True),
            weight * z_centre,
            jnp.zeros((4, cells_z), jnp.float32),
        ],
        axis=0,
    )
    blobs = pair_lanes(moments)
    inverse = 1.0 / blobs[0:1]
    x_index, y_index = here()
    x_anchor = (x_index * cells_x).astype(jnp.float32)
    y_anchor = (y_index * cells_y).astype(jnp.float32)
    row_ref[0:1, :] = (blobs[1:2] * inverse + x_anchor) / cells_z
    row_ref[1:2, :] = (blobs[2:3] * inverse + y_anchor) / cells_z
    row_ref[2:3, :] = (blobs[3:4] * inverse) / cells_z
    alive = lax.broadcasted_iota(jnp.int32, (3, slot_count), 1) < live_ref[0]
    strength = jnp.where(alive, strength_ref[...], 0.0)
    parts = [position_ref[k : k + 1] for k in range(3)] + [strength[k : k + 1] for k in range(3)]
    for k in range(3):
        row_ref[3 + k : 4 + k, :] = jnp.concatenate(parts[2 * k : 2 * k + 2], axis=1)


def block_kernel(sums_ref, wx_ref, wy_ref, row_ref, xa_ref, xb_ref, ya_ref, yb_ref, out_ref):
    x_index, y_index = here()
    x_even = lax.rem(x_index, 2) == 0
    y_even = lax.rem(y_index, 2) == 0
    total = sums_ref[...]
    rows = []
    for k in range(3):
        first = jnp.where(x_even, xb_ref[k], xa_ref[k])
        last = jnp.where(x_even, xa_ref[k], xb_ref[k])
        row = jnp.sum(wx_ref[0] * first + wx_ref[1] * last, axis=0, keepdims=True)
        first = jnp.where(y_even, yb_ref[k], ya_ref[k])
        last = jnp.where(y_even, ya_ref[k], yb_ref[k])
        row = row + jnp.sum(wy_ref[0] * first + wy_ref[1] * last, axis=0, keepdims=True)
        rows.append(row)
    total = total + jnp.concatenate(rows + [jnp.zeros((5, total.shape[1]), jnp.float32)], axis=0)
    strength = seed_weight * pair_lanes(total)
    block = jnp.concatenate([row_ref[0:3], strength[0:3], row_ref[3:6]], axis=0)
    devices = out_ref.shape[0] // GROUPS
    for device in range(devices):
        out_ref[device * GROUPS : (device + 1) * GROUPS, :] = block


def target_rows(own):
    rows = []
    for k in range(3):
        row = own[6 + k : 7 + k]
        rows.append(row)
        rows.append(pltpu.roll(row, LANES // 2, 1))
    return rows


def grid_kernel(v_ref, d_ref, xa_ref, xb_ref, ya_ref, yb_ref, own_ref, out_ref, column_ref):
    _, cells_x, cells_y, cells_z = v_ref.shape
    x_index, y_index = here()
    x_even = lax.rem(x_index, 2) == 0
    y_even = lax.rem(y_index, 2) == 0
    rows = lax.broadcasted_iota(jnp.int32, (cells_y, cells_z), 0)
    for k in range(3):
        before = jnp.where(x_even, xb_ref[k], xa_ref[k])
        beyond = jnp.where(x_even, xa_ref[k], xb_ref[k])
        first = jnp.where(y_even, yb_ref[k], ya_ref[k])
        last = jnp.where(y_even, ya_ref[k], yb_ref[k])
        for x in range(cells_x):
            v = v_ref[k, x]
            low = before if x == 0 else v_ref[k, x - 1]
            high = beyond if x == cells_x - 1 else v_ref[k, x + 1]
            left = jnp.where(rows == 0, first[x : x + 1], pltpu.roll(v, 1, 0))
            right = jnp.where(rows == cells_y - 1, last[x : x + 1], pltpu.roll(v, cells_y - 1, 0))
            beside = (high + low) + (right + left) + (shifted_lanes(v, -1) + shifted_lanes(v, 1))
            out_ref[k, x] = v + d_ref[x] * (beside - 6.0 * v)

    own = own_ref[0:GROUPS, :]
    particles = target_rows(own)
    zeros = jnp.zeros((1, LANES), jnp.float32)
    wide = [jnp.concatenate([own[k : k + 1], particles[k]], axis=1) for k in range(3)]
    wide = wide + [jnp.concatenate([zeros, particles[k]], axis=1) for k in range(3, 6)]
    table = jnp.concatenate(wide + [jnp.zeros((LANES - 6, 2 * LANES), jnp.float32)], axis=0)
    columns = jnp.transpose(table)
    targets = column_ref.shape[1]
    for k in range(6):
        begin = 0 if k < 3 else LANES
        column_ref[k, begin:targets, :] = jnp.broadcast_to(columns[begin:targets, k : k + 1], (targets - begin, LANES))


def pair_kernel(live_ref, all_ref, own_ref, column_ref, rates_ref, blob_ref, source_ref, feature_ref, turn_ref, k_ref, sum_ref, *, cells):
    devices = all_ref.shape[0] // GROUPS
    half = LANES // 2
    tiles = devices + devices // 2
    targets = column_ref.shape[1]
    lane = lax.broadcasted_iota(jnp.int32, (devices, LANES), 1)
    x_index, y_index = here()
    centre = [
        (x_index.astype(jnp.float32) + 0.5) * (cells[0] / cells[2]),
        (y_index.astype(jnp.float32) + 0.5) * (cells[1] / cells[2]),
        0.5,
    ]

    def group(index):
        return all_ref[pl.ds(index, devices, stride=GROUPS), :]

    def evens(rows):
        turn_ref[...] = rows
        return turn_ref[pl.ds(0, devices // 2, stride=2), :]

    blobs = [group(k) for k in range(6)]
    particles = []
    for k in range(3):
        both = group(6 + k)
        turned = pltpu.roll(both, half, 1)
        particles.append(evens(jnp.where(lane < half, both, pltpu.roll(turned, devices - 1, 0))))
        particles.append(evens(jnp.where(lane < half, turned, pltpu.roll(both, devices - 1, 0))))
    elements = [jnp.concatenate([blobs[k], particles[k]], axis=0) for k in range(6)]
    for k in range(3):
        source_ref[k * tiles : (k + 1) * tiles, :] = elements[k]
    place = [elements[k] - centre[k] for k in range(3)]
    a = elements[3:]
    features = a + [
        place[1] * a[2] - place[2] * a[1],
        place[2] * a[0] - place[0] * a[2],
        place[0] * a[1] - place[1] * a[0],
    ]
    feature_ref[...] = jnp.zeros_like(feature_ref)
    for k in range(6):
        parts = split3(features[k])
        for j in range(3):
            row = (8 * j + k) * tiles
            feature_ref[row : row + tiles, :] = parts[j].astype(jnp.float32)

    sum_ref[...] = jnp.zeros_like(sum_ref)
    block = LANES // 2
    width = 4 if tiles % 4 == 0 else 1
    unroll = 4 if tiles % (4 * width) == 0 else 1
    contract = (((1,), (1,)), ((), ()))

    def one(chunk, slot):
        feature = []
        for j in range(width):
            tile = chunk * width + j
            feature.append(feature_ref[pl.ds(tile, 32, stride=tiles), :].astype(jnp.bfloat16))
            source = [source_ref[pl.ds(k * tiles + tile, 1), :] for k in range(3)]
            span = slice(j * LANES, (j + 1) * LANES)
            for t in range(0, targets, block):
                sep = [column_ref[k, t : t + block, :] - source[k] for k in range(3)]
                squared = sep[0] * sep[0] + sep[1] * sep[1] + (sep[2] * sep[2] + sigma_sq)
                inverse = lax.rsqrt(squared)
                square = inverse * inverse
                kernel = square * inverse
                high = kernel.astype(jnp.bfloat16)
                k_ref[slot, t : t + block, span] = high
                k_ref[slot, targets + t : targets + t + block, span] = (kernel - high.astype(jnp.float32)).astype(jnp.bfloat16)
                if t >= LANES:
                    along = column_ref[3, t : t + block, :] * sep[0] + column_ref[4, t : t + block, :] * sep[1] + column_ref[5, t : t + block, :] * sep[2]
                    weighted = (kernel * square) * along
                    high = weighted.astype(jnp.bfloat16)
                    k_ref[slot, 2 * targets : 2 * targets + block, span] = high
                    k_ref[slot, 2 * targets + block : 2 * targets + 2 * block, span] = (weighted - high.astype(jnp.float32)).astype(jnp.bfloat16)
        feature = jnp.concatenate(feature, axis=1)
        sum_ref[:, 0:32] = sum_ref[:, 0:32] + lax.dot_general(k_ref[slot], feature, contract, preferred_element_type=jnp.float32)

    def step(index, _):
        for j in range(unroll):
            one(index * unroll + j, j % 2)
        return 0

    lax.fori_loop(0, tiles // (width * unroll), step, 0)

    def combined(table):
        turned = jnp.transpose(table)
        return turned[0:8] + turned[8:16] + turned[16:24]

    found = combined(jnp.concatenate([sum_ref[0:targets] + sum_ref[targets : 2 * targets], jnp.zeros((block, LANES), jnp.float32)], axis=0))
    pulled = combined(jnp.concatenate([sum_ref[2 * targets : 2 * targets + block] + sum_ref[2 * targets + block :], jnp.zeros((block, LANES), jnp.float32)], axis=0))

    def crossed(place, rows):
        return [
            place[1] * rows[2:3] - place[2] * rows[1:2] - rows[3:4],
            place[2] * rows[0:1] - place[0] * rows[2:3] - rows[4:5],
            place[0] * rows[1:2] - place[1] * rows[0:1] - rows[5:6],
        ]

    own = own_ref[0:GROUPS, :]
    slots = target_rows(own)
    near = found[:, LANES:]
    alive = (lax.broadcasted_iota(jnp.int32, (1, LANES), 1) < live_ref[0]).astype(jnp.float32)
    blob_place = [own[k : k + 1] - centre[k] for k in range(3)]
    slot_place = [slots[k] - centre[k] for k in range(3)]
    a = slots[3:]
    first = [
        a[1] * near[2:3] - a[2] * near[1:2],
        a[2] * near[0:1] - a[0] * near[2:3],
        a[0] * near[1:2] - a[1] * near[0:1],
    ]
    blob_velocity = crossed(blob_place, found[:, 0:LANES])
    slot_velocity = crossed(slot_place, near)
    second = crossed(slot_place, pulled)
    for k in range(3):
        blob_ref[k : k + 1, :] = -kernel_scale * blob_velocity[k]
        rates_ref[k : k + 1, :] = (-kernel_scale * slot_velocity[k] * alive)[:, 0:half]
        rates_ref[3 + k : 4 + k, :] = (-kernel_scale * (first[k] - 3.0 * second[k]) * alive)[:, 0:half]


def partners(count, start):
    pairs = [(i, i + 1) for i in range(start, count - 1, 2)]
    return pairs + [(j, i) for i, j in pairs]


def per_device(positions, strengths, live_counts, vorticity, diffusivity, seed_counts):
    _, cells_x, cells_y, cells_z = vorticity.shape
    slot_count = positions.shape[1]
    y_axes = ("src", "grp")
    everyone = ("tgt", "src", "grp")
    x_count, y_count = lax.axis_size("tgt"), lax.axis_size("src") * lax.axis_size("grp")
    devices = x_count * y_count
    f32 = jnp.float32

    def kept(*shape):
        return pltpu.VMEM(shape, f32)

    def held(array):
        return pltpu.with_memory_space_constraint(array, pltpu.VMEM)

    xa, xb, ya, yb = pl.pallas_call(
        faces_kernel,
        name="faces",
        out_shape=(kept(3, cells_y, cells_z), kept(3, cells_y, cells_z), kept(3, cells_x, cells_z), kept(3, cells_x, cells_z)),
        in_specs=[pl.BlockSpec(memory_space=pl.ANY)],
        out_specs=[VMEM] * 4,
        scratch_shapes=[
            pltpu.VMEM((3, cells_x, 8, cells_z), f32),
            pltpu.VMEM((3, cells_x, 8, cells_z), f32),
            pltpu.SemaphoreType.DMA((4,)),
        ],
    )(vorticity)
    xa = held(lax.ppermute(xa, "tgt", partners(x_count, 0)))
    xb = held(lax.ppermute(xb, "tgt", partners(x_count, 1)))
    ya = held(lax.ppermute(ya, y_axes, partners(y_count, 0)))
    yb = held(lax.ppermute(yb, y_axes, partners(y_count, 1)))

    v, d, c = held(vorticity), diffusivity, seed_counts
    sums, wx, wy, rows = pl.pallas_call(
        local_kernel,
        name="local",
        out_shape=(kept(8, cells_z), kept(2, cells_y, cells_z), kept(2, cells_x, cells_z), kept(8, LANES)),
        in_specs=[SMEM] + [VMEM] * 5,
        out_specs=[VMEM] * 4,
    )(live_counts, v, d, c, positions, strengths)
    block = pl.pallas_call(
        block_kernel,
        name="block",
        out_shape=kept(devices * GROUPS, LANES),
        in_specs=[VMEM] * 8,
        out_specs=VMEM,
    )(held(sums), held(wx), held(wy), held(rows), xa, xb, ya, yb)
    everything = lax.all_to_all(block.reshape(-1), everyone, 0, 0, tiled=True).reshape(devices * GROUPS, LANES)

    targets = LANES + slot_count
    vorticity_next, columns = pl.pallas_call(
        grid_kernel,
        name="grid",
        out_shape=(jax.ShapeDtypeStruct(vorticity.shape, f32), kept(6, targets, LANES)),
        in_specs=[VMEM] * 7,
        out_specs=[VMEM] * 2,
    )(v, d, xa, xb, ya, yb, held(block))

    tiles = devices + devices // 2
    width = 4 if tiles % 4 == 0 else 1
    particle_rates, blob_velocity = pl.pallas_call(
        functools.partial(pair_kernel, cells=(cells_x, cells_y, cells_z)),
        name="pairs",
        out_shape=(jax.ShapeDtypeStruct((6, slot_count), f32), jax.ShapeDtypeStruct((3, LANES), f32)),
        in_specs=[SMEM] + [VMEM] * 3,
        out_specs=[VMEM, VMEM],
        scratch_shapes=[
            pltpu.VMEM((3 * tiles, LANES), f32),
            pltpu.VMEM((32 * tiles, LANES), f32),
            pltpu.VMEM((devices, LANES), f32),
            pltpu.VMEM((2, 2 * targets + 2 * slot_count, width * LANES), jnp.bfloat16),
            pltpu.VMEM((2 * targets + 2 * slot_count, LANES), f32),
        ],
    )(live_counts, held(everything), held(block), held(columns))
    return (vorticity_next, particle_rates, blob_velocity)


def solution(mesh):
    placed = (
        P(None, ("tgt", "src", "grp")),
        P(None, ("tgt", "src", "grp")),
        P(("tgt", "src", "grp")),
        P(None, "tgt", ("src", "grp"), None),
        P("tgt", ("src", "grp"), None),
        P("tgt", ("src", "grp"), None),
    )
    return jax.shard_map(
        per_device,
        mesh=mesh,
        in_specs=placed,
        out_specs=(
            P(None, "tgt", ("src", "grp"), None),
            P(None, ("tgt", "src", "grp")),
            P(None, ("tgt", "src", "grp")),
        ),
        check_vma=False,
    )
```

```python
import functools
import jax
import jax.numpy as jnp
from jax import lax
from jax.experimental import pallas as pl
from jax.experimental.pallas import tpu as pltpu
from jax.sharding import PartitionSpec as P

BZ = 2
LANES = 128
GROUPS = 9

sigma_sq = 0.0004
kernel_scale = 0.25 / 3.141592653589793
seed_weight = 0.0001


VMEM = pl.BlockSpec(memory_space=pltpu.VMEM)
SMEM = pl.BlockSpec(memory_space=pltpu.SMEM)


def split3(value):
    high = value.astype(jnp.bfloat16)
    rest = value - high.astype(jnp.float32)
    middle = rest.astype(jnp.bfloat16)
    low = (rest - middle.astype(jnp.float32)).astype(jnp.bfloat16)
    return high, middle, low


def pair_lanes(rows):
    length = rows.shape[1]
    cell = lax.broadcasted_iota(jnp.int32, (length, length // BZ), 0)
    blob = lax.broadcasted_iota(jnp.int32, (length, length // BZ), 1)
    chosen = jnp.where((cell >= blob * BZ) & (cell < blob * BZ + BZ), 1.0, 0.0).astype(jnp.bfloat16)
    total = None
    for part in split3(rows):
        product = jnp.dot(part, chosen, preferred_element_type=jnp.float32)
        total = product if total is None else total + product
    return total


def shifted_rows(value, step):
    rows = lax.broadcasted_iota(jnp.int32, value.shape, 0)
    count = value.shape[0]
    if step == 1:
        return jnp.where(rows == 0, 0.0, pltpu.roll(value, 1, 0))
    return jnp.where(rows == count - 1, 0.0, pltpu.roll(value, count - 1, 0))


def shifted_lanes(value, step):
    lanes = lax.broadcasted_iota(jnp.int32, value.shape, 1)
    count = value.shape[1]
    if step == 1:
        return jnp.where(lanes == 0, 0.0, pltpu.roll(value, 1, 1))
    return jnp.where(lanes == count - 1, 0.0, pltpu.roll(value, count - 1, 1))


def here():
    x_index = lax.axis_index("tgt")
    y_index = lax.axis_index("src") * lax.axis_size("grp") + lax.axis_index("grp")
    return x_index, y_index


def faces_kernel(v_ref, xa_ref, xb_ref, ya_ref, yb_ref, low_ref, high_ref, sems):
    _, cells_x, cells_y, _ = v_ref.shape
    x_index, y_index = here()
    x_even = lax.rem(x_index, 2) == 0
    y_even = lax.rem(y_index, 2) == 0
    top = (cells_y - 1) // 8 * 8
    last = cells_x - 1
    copies = [
        pltpu.make_async_copy(v_ref.at[:, jnp.where(x_even, 0, last)], xb_ref, sems.at[0]),
        pltpu.make_async_copy(v_ref.at[:, jnp.where(x_even, last, 0)], xa_ref, sems.at[1]),
        pltpu.make_async_copy(v_ref.at[:, :, 0:8], low_ref, sems.at[2]),
        pltpu.make_async_copy(v_ref.at[:, :, top : top + 8], high_ref, sems.at[3]),
    ]
    for copy in copies:
        copy.start()
    copies[2].wait()
    copies[3].wait()
    for k in range(3):
        first = low_ref[k, :, 0, :]
        final = high_ref[k, :, cells_y - 1 - top, :]
        ya_ref[k] = jnp.where(y_even, final, first)
        yb_ref[k] = jnp.where(y_even, first, final)
    copies[0].wait()
    copies[1].wait()


def local_kernel(live_ref, v_ref, d_ref, c_ref, position_ref, strength_ref, sums_ref, wx_ref, wy_ref, row_ref):
    _, cells_x, cells_y, cells_z = v_ref.shape
    slot_count = position_ref.shape[1]
    w = []
    c = []
    for x in range(cells_x):
        counts = c_ref[x].astype(jnp.float32)
        c.append(counts)
        w.append(counts * d_ref[x])
    wx_ref[0] = w[0]
    wx_ref[1] = w[cells_x - 1]
    for x in range(cells_x):
        wy_ref[0, x : x + 1, :] = w[x][0:1, :]
        wy_ref[1, x : x + 1, :] = w[x][cells_y - 1 : cells_y, :]
    zero = jnp.zeros((cells_y, cells_z), jnp.float32)
    at = [zero] * 3
    after = [zero] * 3
    before = [zero] * 3
    plain = zero
    moment = zero
    for x in range(cells_x):
        beside = shifted_rows(w[x], 1) + shifted_rows(w[x], -1)
        if x > 0:
            beside = beside + w[x - 1]
        if x < cells_x - 1:
            beside = beside + w[x + 1]
        around = c[x] + (beside - 6.0 * w[x])
        up = shifted_lanes(w[x], 1)
        down = shifted_lanes(w[x], -1)
        for k in range(3):
            v = v_ref[k, x]
            at[k] = at[k] + around * v
            after[k] = after[k] + up * v
            before[k] = before[k] + down * v
        plain = plain + (c[x] + 1.0)
        moment = moment + (c[x] + 1.0) * (x + 0.5)
    rows = []
    for k in range(3):
        total = (
            jnp.sum(at[k], axis=0, keepdims=True)
            + shifted_lanes(jnp.sum(after[k], axis=0, keepdims=True), -1)
            + shifted_lanes(jnp.sum(before[k], axis=0, keepdims=True), 1)
        )
        rows.append(total)
    sums_ref[0:3, :] = jnp.concatenate(rows, axis=0)
    sums_ref[3:8, :] = jnp.zeros((5, cells_z), jnp.float32)
    y_centre = lax.broadcasted_iota(jnp.int32, (cells_y, cells_z), 0).astype(jnp.float32) + 0.5
    z_centre = lax.broadcasted_iota(jnp.int32, (1, cells_z), 1).astype(jnp.float32) + 0.5
    weight = jnp.sum(plain, axis=0, keepdims=True)
    moments = jnp.concatenate(
        [
            weight,
            jnp.sum(moment, axis=0, keepdims=True),
            jnp.sum(plain * y_centre, axis=0, keepdims=True),
            weight * z_centre,
            jnp.zeros((4, cells_z), jnp.float32),
        ],
        axis=0,
    )
    blobs = pair_lanes(moments)
    inverse = 1.0 / blobs[0:1]
    x_index, y_index = here()
    x_anchor = (x_index * cells_x).astype(jnp.float32)
    y_anchor = (y_index * cells_y).astype(jnp.float32)
    row_ref[0:1, :] = (blobs[1:2] * inverse + x_anchor) / cells_z
    row_ref[1:2, :] = (blobs[2:3] * inverse + y_anchor) / cells_z
    row_ref[2:3, :] = (blobs[3:4] * inverse) / cells_z
    alive = lax.broadcasted_iota(jnp.int32, (3, slot_count), 1) < live_ref[0]
    strength = jnp.where(alive, strength_ref[...], 0.0)
    parts = [position_ref[k : k + 1] for k in range(3)] + [strength[k : k + 1] for k in range(3)]
    for k in range(3):
        row_ref[3 + k : 4 + k, :] = jnp.concatenate(parts[2 * k : 2 * k + 2], axis=1)


def block_kernel(sums_ref, wx_ref, wy_ref, row_ref, xa_ref, xb_ref, ya_ref, yb_ref, out_ref):
    x_index, y_index = here()
    x_even = lax.rem(x_index, 2) == 0
    y_even = lax.rem(y_index, 2) == 0
    total = sums_ref[...]
    rows = []
    for k in range(3):
        first = jnp.where(x_even, xb_ref[k], xa_ref[k])
        last = jnp.where(x_even, xa_ref[k], xb_ref[k])
        row = jnp.sum(wx_ref[0] * first + wx_ref[1] * last, axis=0, keepdims=True)
        first = jnp.where(y_even, yb_ref[k], ya_ref[k])
        last = jnp.where(y_even, ya_ref[k], yb_ref[k])
        row = row + jnp.sum(wy_ref[0] * first + wy_ref[1] * last, axis=0, keepdims=True)
        rows.append(row)
    total = total + jnp.concatenate(rows + [jnp.zeros((5, total.shape[1]), jnp.float32)], axis=0)
    strength = seed_weight * pair_lanes(total)
    block = jnp.concatenate([row_ref[0:3], strength[0:3], row_ref[3:6]], axis=0)
    devices = out_ref.shape[0] // GROUPS
    for device in range(devices):
        out_ref[device * GROUPS : (device + 1) * GROUPS, :] = block


def target_rows(own):
    rows = []
    for k in range(3):
        row = own[6 + k : 7 + k]
        rows.append(row)
        rows.append(pltpu.roll(row, LANES // 2, 1))
    return rows


def grid_kernel(v_ref, d_ref, xa_ref, xb_ref, ya_ref, yb_ref, own_ref, out_ref, column_ref):
    _, cells_x, cells_y, cells_z = v_ref.shape
    x_index, y_index = here()
    x_even = lax.rem(x_index, 2) == 0
    y_even = lax.rem(y_index, 2) == 0
    rows = lax.broadcasted_iota(jnp.int32, (cells_y, cells_z), 0)
    for k in range(3):
        before = jnp.where(x_even, xb_ref[k], xa_ref[k])
        beyond = jnp.where(x_even, xa_ref[k], xb_ref[k])
        first = jnp.where(y_even, yb_ref[k], ya_ref[k])
        last = jnp.where(y_even, ya_ref[k], yb_ref[k])
        for x in range(cells_x):
            v = v_ref[k, x]
            low = before if x == 0 else v_ref[k, x - 1]
            high = beyond if x == cells_x - 1 else v_ref[k, x + 1]
            left = jnp.where(rows == 0, first[x : x + 1], pltpu.roll(v, 1, 0))
            right = jnp.where(rows == cells_y - 1, last[x : x + 1], pltpu.roll(v, cells_y - 1, 0))
            beside = (high + low) + (right + left) + (shifted_lanes(v, -1) + shifted_lanes(v, 1))
            out_ref[k, x] = v + d_ref[x] * (beside - 6.0 * v)

    own = own_ref[0:GROUPS, :]
    particles = target_rows(own)
    zeros = jnp.zeros((1, LANES), jnp.float32)
    wide = [jnp.concatenate([own[k : k + 1], particles[k]], axis=1) for k in range(3)]
    wide = wide + [jnp.concatenate([zeros, particles[k]], axis=1) for k in range(3, 6)]
    table = jnp.concatenate(wide + [jnp.zeros((LANES - 6, 2 * LANES), jnp.float32)], axis=0)
    columns = jnp.transpose(table)
    targets = column_ref.shape[1]
    for k in range(6):
        begin = 0 if k < 3 else LANES
        column_ref[k, begin:targets, :] = jnp.broadcast_to(columns[begin:targets, k : k + 1], (targets - begin, LANES))


def pair_kernel(live_ref, all_ref, own_ref, column_ref, rates_ref, blob_ref, source_ref, feature_ref, turn_ref, sum_ref, *, cells):
    devices = all_ref.shape[0] // GROUPS
    half = LANES // 2
    tiles = devices + devices // 2
    targets = column_ref.shape[1]
    lane = lax.broadcasted_iota(jnp.int32, (devices, LANES), 1)
    x_index, y_index = here()
    centre = [
        (x_index.astype(jnp.float32) + 0.5) * (cells[0] / cells[2]),
        (y_index.astype(jnp.float32) + 0.5) * (cells[1] / cells[2]),
        0.5,
    ]

    def group(index):
        return all_ref[pl.ds(index, devices, stride=GROUPS), :]

    def evens(rows):
        turn_ref[...] = rows
        return turn_ref[pl.ds(0, devices // 2, stride=2), :]

    blobs = [group(k) for k in range(6)]
    particles = []
    for k in range(3):
        both = group(6 + k)
        turned = pltpu.roll(both, half, 1)
        particles.append(evens(jnp.where(lane < half, both, pltpu.roll(turned, devices - 1, 0))))
        particles.append(evens(jnp.where(lane < half, turned, pltpu.roll(both, devices - 1, 0))))
    elements = [jnp.concatenate([blobs[k], particles[k]], axis=0) for k in range(6)]
    for k in range(3):
        source_ref[k * tiles : (k + 1) * tiles, :] = elements[k]
    place = [elements[k] - centre[k] for k in range(3)]
    a = elements[3:]
    features = a + [
        place[1] * a[2] - place[2] * a[1],
        place[2] * a[0] - place[0] * a[2],
        place[0] * a[1] - place[1] * a[0],
    ]
    feature_ref[...] = jnp.zeros_like(feature_ref)
    for k in range(6):
        parts = split3(features[k])
        for j in range(3):
            row = (8 * j + k) * tiles
            feature_ref[row : row + tiles, :] = parts[j].astype(jnp.float32)

    sum_ref[...] = jnp.zeros_like(sum_ref)
    block = 32
    width = 4 if tiles % 4 == 0 else 1
    unroll = 4 if tiles % (4 * width) == 0 else 1
    contract = (((1,), (1,)), ((), ()))

    def product(values, feature):
        highs = [value.astype(jnp.bfloat16) for value in values]
        lows = [(value - high.astype(jnp.float32)).astype(jnp.bfloat16) for value, high in zip(values, highs)]
        both = jnp.concatenate([jnp.concatenate(highs, axis=1), jnp.concatenate(lows, axis=1)], axis=0)
        return lax.dot_general(both, feature, contract, preferred_element_type=jnp.float32)

    def one(chunk):
        spans = [chunk * width + j for j in range(width)]
        feature = jnp.concatenate([feature_ref[pl.ds(tile, 32, stride=tiles), :].astype(jnp.bfloat16) for tile in spans], axis=1)
        source = [[source_ref[pl.ds(k * tiles + tile, 1), :] for k in range(3)] for tile in spans]
        for t in range(0, targets, block):
            kernels, pulls = [], []
            for j in range(width):
                sep = [column_ref[k, t : t + block, :] - source[j][k] for k in range(3)]
                squared = sep[0] * sep[0] + sep[1] * sep[1] + (sep[2] * sep[2] + sigma_sq)
                inverse = lax.rsqrt(squared)
                square = inverse * inverse
                kernel = square * inverse
                kernels.append(kernel)
                if t >= LANES:
                    along = column_ref[3, t : t + block, :] * sep[0] + column_ref[4, t : t + block, :] * sep[1] + column_ref[5, t : t + block, :] * sep[2]
                    pulls.append((kernel * square) * along)
            rows = slice(2 * t, 2 * t + 2 * block)
            sum_ref[rows, 0:32] = sum_ref[rows, 0:32] + product(kernels, feature)
            if t >= LANES:
                rows = slice(2 * (targets + t - LANES), 2 * (targets + t - LANES) + 2 * block)
                sum_ref[rows, 0:32] = sum_ref[rows, 0:32] + product(pulls, feature)

    def step(index, _):
        for j in range(unroll):
            one(index * unroll + j)
        return 0

    lax.fori_loop(0, tiles // (width * unroll), step, 0)

    def combined(begin, end):
        parts = [sum_ref[2 * t : 2 * t + block] + sum_ref[2 * t + block : 2 * t + 2 * block] for t in range(begin, end, block)]
        rest = -(end - begin) % LANES
        if rest:
            parts.append(jnp.zeros((rest, LANES), jnp.float32))
        turned = jnp.transpose(jnp.concatenate(parts, axis=0))
        return turned[0:8] + turned[8:16] + turned[16:24]

    found = combined(0, targets)
    pulled = combined(targets, targets + half)

    def crossed(place, rows):
        return [
            place[1] * rows[2:3] - place[2] * rows[1:2] - rows[3:4],
            place[2] * rows[0:1] - place[0] * rows[2:3] - rows[4:5],
            place[0] * rows[1:2] - place[1] * rows[0:1] - rows[5:6],
        ]

    own = own_ref[0:GROUPS, :]
    slots = target_rows(own)
    near = found[:, LANES:]
    alive = (lax.broadcasted_iota(jnp.int32, (1, LANES), 1) < live_ref[0]).astype(jnp.float32)
    blob_place = [own[k : k + 1] - centre[k] for k in range(3)]
    slot_place = [slots[k] - centre[k] for k in range(3)]
    a = slots[3:]
    first = [
        a[1] * near[2:3] - a[2] * near[1:2],
        a[2] * near[0:1] - a[0] * near[2:3],
        a[0] * near[1:2] - a[1] * near[0:1],
    ]
    blob_velocity = crossed(blob_place, found[:, 0:LANES])
    slot_velocity = crossed(slot_place, near)
    second = crossed(slot_place, pulled)
    for k in range(3):
        blob_ref[k : k + 1, :] = -kernel_scale * blob_velocity[k]
        rates_ref[k : k + 1, :] = (-kernel_scale * slot_velocity[k] * alive)[:, 0:half]
        rates_ref[3 + k : 4 + k, :] = (-kernel_scale * (first[k] - 3.0 * second[k]) * alive)[:, 0:half]


def partners(count, start):
    pairs = [(i, i + 1) for i in range(start, count - 1, 2)]
    return pairs + [(j, i) for i, j in pairs]


def per_device(positions, strengths, live_counts, vorticity, diffusivity, seed_counts):
    _, cells_x, cells_y, cells_z = vorticity.shape
    slot_count = positions.shape[1]
    y_axes = ("src", "grp")
    everyone = ("tgt", "src", "grp")
    x_count, y_count = lax.axis_size("tgt"), lax.axis_size("src") * lax.axis_size("grp")
    devices = x_count * y_count
    f32 = jnp.float32

    def kept(*shape):
        return pltpu.VMEM(shape, f32)

    def held(array):
        return pltpu.with_memory_space_constraint(array, pltpu.VMEM)

    xa, xb, ya, yb = pl.pallas_call(
        faces_kernel,
        name="faces",
        out_shape=(kept(3, cells_y, cells_z), kept(3, cells_y, cells_z), kept(3, cells_x, cells_z), kept(3, cells_x, cells_z)),
        in_specs=[pl.BlockSpec(memory_space=pl.ANY)],
        out_specs=[VMEM] * 4,
        scratch_shapes=[
            pltpu.VMEM((3, cells_x, 8, cells_z), f32),
            pltpu.VMEM((3, cells_x, 8, cells_z), f32),
            pltpu.SemaphoreType.DMA((4,)),
        ],
    )(vorticity)
    xa = held(lax.ppermute(xa, "tgt", partners(x_count, 0)))
    xb = held(lax.ppermute(xb, "tgt", partners(x_count, 1)))
    ya = held(lax.ppermute(ya, y_axes, partners(y_count, 0)))
    yb = held(lax.ppermute(yb, y_axes, partners(y_count, 1)))

    v, d, c = held(vorticity), diffusivity, seed_counts
    sums, wx, wy, rows = pl.pallas_call(
        local_kernel,
        name="local",
        out_shape=(kept(8, cells_z), kept(2, cells_y, cells_z), kept(2, cells_x, cells_z), kept(8, LANES)),
        in_specs=[SMEM] + [VMEM] * 5,
        out_specs=[VMEM] * 4,
    )(live_counts, v, d, c, positions, strengths)
    block = pl.pallas_call(
        block_kernel,
        name="block",
        out_shape=kept(devices * GROUPS, LANES),
        in_specs=[VMEM] * 8,
        out_specs=VMEM,
    )(held(sums), held(wx), held(wy), held(rows), xa, xb, ya, yb)
    everything = lax.all_to_all(block.reshape(-1), everyone, 0, 0, tiled=True).reshape(devices * GROUPS, LANES)

    targets = LANES + slot_count
    vorticity_next, columns = pl.pallas_call(
        grid_kernel,
        name="grid",
        out_shape=(jax.ShapeDtypeStruct(vorticity.shape, f32), kept(6, targets, LANES)),
        in_specs=[VMEM] * 7,
        out_specs=[VMEM] * 2,
    )(v, d, xa, xb, ya, yb, held(block))

    tiles = devices + devices // 2
    particle_rates, blob_velocity = pl.pallas_call(
        functools.partial(pair_kernel, cells=(cells_x, cells_y, cells_z)),
        name="pairs",
        out_shape=(jax.ShapeDtypeStruct((6, slot_count), f32), jax.ShapeDtypeStruct((3, LANES), f32)),
        in_specs=[SMEM] + [VMEM] * 3,
        out_specs=[VMEM, VMEM],
        scratch_shapes=[
            pltpu.VMEM((3 * tiles, LANES), f32),
            pltpu.VMEM((32 * tiles, LANES), f32),
            pltpu.VMEM((devices, LANES), f32),
            pltpu.VMEM((2 * targets + 2 * slot_count, LANES), f32),
        ],
    )(live_counts, held(everything), held(block), held(columns))
    return (vorticity_next, particle_rates, blob_velocity)


def solution(mesh):
    placed = (
        P(None, ("tgt", "src", "grp")),
        P(None, ("tgt", "src", "grp")),
        P(("tgt", "src", "grp")),
        P(None, "tgt", ("src", "grp"), None),
        P("tgt", ("src", "grp"), None),
        P("tgt", ("src", "grp"), None),
    )
    return jax.shard_map(
        per_device,
        mesh=mesh,
        in_specs=placed,
        out_specs=(
            P(None, "tgt", ("src", "grp"), None),
            P(None, ("tgt", "src", "grp")),
            P(None, ("tgt", "src", "grp")),
        ),
        check_vma=False,
    )
```

```python
import functools
import jax
import jax.numpy as jnp
from jax import lax
from jax.experimental import pallas as pl
from jax.experimental.pallas import tpu as pltpu
from jax.sharding import PartitionSpec as P

BZ = 2
LANES = 128
GROUPS = 9

sigma_sq = 0.0004
kernel_scale = 0.25 / 3.141592653589793
seed_weight = 0.0001


VMEM = pl.BlockSpec(memory_space=pltpu.VMEM)
SMEM = pl.BlockSpec(memory_space=pltpu.SMEM)


def split3(value):
    high = value.astype(jnp.bfloat16)
    rest = value - high.astype(jnp.float32)
    middle = rest.astype(jnp.bfloat16)
    low = (rest - middle.astype(jnp.float32)).astype(jnp.bfloat16)
    return high, middle, low


def pair_lanes(rows):
    length = rows.shape[1]
    cell = lax.broadcasted_iota(jnp.int32, (length, length // BZ), 0)
    blob = lax.broadcasted_iota(jnp.int32, (length, length // BZ), 1)
    chosen = jnp.where((cell >= blob * BZ) & (cell < blob * BZ + BZ), 1.0, 0.0).astype(jnp.bfloat16)
    total = None
    for part in split3(rows):
        product = jnp.dot(part, chosen, preferred_element_type=jnp.float32)
        total = product if total is None else total + product
    return total


def shifted_rows(value, step):
    rows = lax.broadcasted_iota(jnp.int32, value.shape, 0)
    count = value.shape[0]
    if step == 1:
        return jnp.where(rows == 0, 0.0, pltpu.roll(value, 1, 0))
    return jnp.where(rows == count - 1, 0.0, pltpu.roll(value, count - 1, 0))


def shifted_lanes(value, step):
    lanes = lax.broadcasted_iota(jnp.int32, value.shape, 1)
    count = value.shape[1]
    if step == 1:
        return jnp.where(lanes == 0, 0.0, pltpu.roll(value, 1, 1))
    return jnp.where(lanes == count - 1, 0.0, pltpu.roll(value, count - 1, 1))


def here():
    x_index = lax.axis_index("tgt")
    y_index = lax.axis_index("src") * lax.axis_size("grp") + lax.axis_index("grp")
    return x_index, y_index


def faces_kernel(v_ref, xa_ref, xb_ref, ya_ref, yb_ref, low_ref, high_ref, sems):
    _, cells_x, cells_y, _ = v_ref.shape
    x_index, y_index = here()
    x_even = lax.rem(x_index, 2) == 0
    y_even = lax.rem(y_index, 2) == 0
    top = (cells_y - 1) // 8 * 8
    last = cells_x - 1
    copies = [
        pltpu.make_async_copy(v_ref.at[:, jnp.where(x_even, 0, last)], xb_ref, sems.at[0]),
        pltpu.make_async_copy(v_ref.at[:, jnp.where(x_even, last, 0)], xa_ref, sems.at[1]),
        pltpu.make_async_copy(v_ref.at[:, :, 0:8], low_ref, sems.at[2]),
        pltpu.make_async_copy(v_ref.at[:, :, top : top + 8], high_ref, sems.at[3]),
    ]
    for copy in copies:
        copy.start()
    copies[2].wait()
    copies[3].wait()
    for k in range(3):
        first = low_ref[k, :, 0, :]
        final = high_ref[k, :, cells_y - 1 - top, :]
        ya_ref[k] = jnp.where(y_even, final, first)
        yb_ref[k] = jnp.where(y_even, first, final)
    copies[0].wait()
    copies[1].wait()


def local_kernel(live_ref, v_ref, d_ref, c_ref, position_ref, strength_ref, sums_ref, wx_ref, wy_ref, row_ref):
    _, cells_x, cells_y, cells_z = v_ref.shape
    slot_count = position_ref.shape[1]
    w = []
    c = []
    for x in range(cells_x):
        counts = c_ref[x].astype(jnp.float32)
        c.append(counts)
        w.append(counts * d_ref[x])
    wx_ref[0] = w[0]
    wx_ref[1] = w[cells_x - 1]
    for x in range(cells_x):
        wy_ref[0, x : x + 1, :] = w[x][0:1, :]
        wy_ref[1, x : x + 1, :] = w[x][cells_y - 1 : cells_y, :]
    zero = jnp.zeros((cells_y, cells_z), jnp.float32)
    at = [zero] * 3
    after = [zero] * 3
    before = [zero] * 3
    plain = zero
    moment = zero
    for x in range(cells_x):
        beside = shifted_rows(w[x], 1) + shifted_rows(w[x], -1)
        if x > 0:
            beside = beside + w[x - 1]
        if x < cells_x - 1:
            beside = beside + w[x + 1]
        around = c[x] + (beside - 6.0 * w[x])
        up = shifted_lanes(w[x], 1)
        down = shifted_lanes(w[x], -1)
        for k in range(3):
            v = v_ref[k, x]
            at[k] = at[k] + around * v
            after[k] = after[k] + up * v
            before[k] = before[k] + down * v
        plain = plain + (c[x] + 1.0)
        moment = moment + (c[x] + 1.0) * (x + 0.5)
    rows = []
    for k in range(3):
        total = (
            jnp.sum(at[k], axis=0, keepdims=True)
            + shifted_lanes(jnp.sum(after[k], axis=0, keepdims=True), -1)
            + shifted_lanes(jnp.sum(before[k], axis=0, keepdims=True), 1)
        )
        rows.append(total)
    sums_ref[0:3, :] = jnp.concatenate(rows, axis=0)
    sums_ref[3:8, :] = jnp.zeros((5, cells_z), jnp.float32)
    y_centre = lax.broadcasted_iota(jnp.int32, (cells_y, cells_z), 0).astype(jnp.float32) + 0.5
    z_centre = lax.broadcasted_iota(jnp.int32, (1, cells_z), 1).astype(jnp.float32) + 0.5
    weight = jnp.sum(plain, axis=0, keepdims=True)
    moments = jnp.concatenate(
        [
            weight,
            jnp.sum(moment, axis=0, keepdims=True),
            jnp.sum(plain * y_centre, axis=0, keepdims=True),
            weight * z_centre,
            jnp.zeros((4, cells_z), jnp.float32),
        ],
        axis=0,
    )
    blobs = pair_lanes(moments)
    inverse = 1.0 / blobs[0:1]
    x_index, y_index = here()
    x_anchor = (x_index * cells_x).astype(jnp.float32)
    y_anchor = (y_index * cells_y).astype(jnp.float32)
    row_ref[0:1, :] = (blobs[1:2] * inverse + x_anchor) / cells_z
    row_ref[1:2, :] = (blobs[2:3] * inverse + y_anchor) / cells_z
    row_ref[2:3, :] = (blobs[3:4] * inverse) / cells_z
    alive = lax.broadcasted_iota(jnp.int32, (3, slot_count), 1) < live_ref[0]
    strength = jnp.where(alive, strength_ref[...], 0.0)
    parts = [position_ref[k : k + 1] for k in range(3)] + [strength[k : k + 1] for k in range(3)]
    for k in range(3):
        row_ref[3 + k : 4 + k, :] = jnp.concatenate(parts[2 * k : 2 * k + 2], axis=1)


def block_kernel(sums_ref, wx_ref, wy_ref, row_ref, xa_ref, xb_ref, ya_ref, yb_ref, out_ref, own_ref):
    x_index, y_index = here()
    x_even = lax.rem(x_index, 2) == 0
    y_even = lax.rem(y_index, 2) == 0
    total = sums_ref[...]
    rows = []
    for k in range(3):
        first = jnp.where(x_even, xb_ref[k], xa_ref[k])
        last = jnp.where(x_even, xa_ref[k], xb_ref[k])
        row = jnp.sum(wx_ref[0] * first + wx_ref[1] * last, axis=0, keepdims=True)
        first = jnp.where(y_even, yb_ref[k], ya_ref[k])
        last = jnp.where(y_even, ya_ref[k], yb_ref[k])
        row = row + jnp.sum(wy_ref[0] * first + wy_ref[1] * last, axis=0, keepdims=True)
        rows.append(row)
    total = total + jnp.concatenate(rows + [jnp.zeros((5, total.shape[1]), jnp.float32)], axis=0)
    strength = seed_weight * pair_lanes(total)
    block = jnp.concatenate([row_ref[0:3], strength[0:3], row_ref[3:6]], axis=0)
    own_ref[0:GROUPS, :] = block
    devices = out_ref.shape[0] // GROUPS
    for device in range(devices):
        out_ref[device * GROUPS : (device + 1) * GROUPS, :] = block


def target_rows(own):
    rows = []
    for k in range(3):
        row = own[6 + k : 7 + k]
        rows.append(row)
        rows.append(pltpu.roll(row, LANES // 2, 1))
    return rows


def grid_kernel(v_ref, d_ref, xa_ref, xb_ref, ya_ref, yb_ref, own_ref, out_ref, column_ref):
    _, cells_x, cells_y, cells_z = v_ref.shape
    x_index, y_index = here()
    x_even = lax.rem(x_index, 2) == 0
    y_even = lax.rem(y_index, 2) == 0
    rows = lax.broadcasted_iota(jnp.int32, (cells_y, cells_z), 0)
    for k in range(3):
        before = jnp.where(x_even, xb_ref[k], xa_ref[k])
        beyond = jnp.where(x_even, xa_ref[k], xb_ref[k])
        first = jnp.where(y_even, yb_ref[k], ya_ref[k])
        last = jnp.where(y_even, ya_ref[k], yb_ref[k])
        for x in range(cells_x):
            v = v_ref[k, x]
            low = before if x == 0 else v_ref[k, x - 1]
            high = beyond if x == cells_x - 1 else v_ref[k, x + 1]
            left = jnp.where(rows == 0, first[x : x + 1], pltpu.roll(v, 1, 0))
            right = jnp.where(rows == cells_y - 1, last[x : x + 1], pltpu.roll(v, cells_y - 1, 0))
            beside = (high + low) + (right + left) + (shifted_lanes(v, -1) + shifted_lanes(v, 1))
            out_ref[k, x] = v + d_ref[x] * (beside - 6.0 * v)

    own = own_ref[0:GROUPS, :]
    particles = target_rows(own)
    zeros = jnp.zeros((1, LANES), jnp.float32)
    wide = [jnp.concatenate([own[k : k + 1], particles[k]], axis=1) for k in range(3)]
    wide = wide + [jnp.concatenate([zeros, particles[k]], axis=1) for k in range(3, 6)]
    table = jnp.concatenate(wide + [jnp.zeros((LANES - 6, 2 * LANES), jnp.float32)], axis=0)
    columns = jnp.transpose(table)
    targets = column_ref.shape[1]
    for k in range(6):
        begin = 0 if k < 3 else LANES
        column_ref[k, begin:targets, :] = jnp.broadcast_to(columns[begin:targets, k : k + 1], (targets - begin, LANES))


def pair_kernel(live_ref, all_ref, own_ref, column_ref, rates_ref, blob_ref, source_ref, feature_ref, turn_ref, sum_ref, *, cells):
    devices = all_ref.shape[0] // GROUPS
    half = LANES // 2
    tiles = devices + devices // 2
    targets = column_ref.shape[1]
    lane = lax.broadcasted_iota(jnp.int32, (devices, LANES), 1)
    x_index, y_index = here()
    centre = [
        (x_index.astype(jnp.float32) + 0.5) * (cells[0] / cells[2]),
        (y_index.astype(jnp.float32) + 0.5) * (cells[1] / cells[2]),
        0.5,
    ]

    def group(index):
        return all_ref[pl.ds(index, devices, stride=GROUPS), :]

    def evens(rows):
        turn_ref[...] = rows
        return turn_ref[pl.ds(0, devices // 2, stride=2), :]

    blobs = [group(k) for k in range(6)]
    particles = []
    for k in range(3):
        both = group(6 + k)
        turned = pltpu.roll(both, half, 1)
        particles.append(evens(jnp.where(lane < half, both, pltpu.roll(turned, devices - 1, 0))))
        particles.append(evens(jnp.where(lane < half, turned, pltpu.roll(both, devices - 1, 0))))
    elements = [jnp.concatenate([blobs[k], particles[k]], axis=0) for k in range(6)]
    for k in range(3):
        source_ref[k * tiles : (k + 1) * tiles, :] = elements[k]
    place = [elements[k] - centre[k] for k in range(3)]
    a = elements[3:]
    features = a + [
        place[1] * a[2] - place[2] * a[1],
        place[2] * a[0] - place[0] * a[2],
        place[0] * a[1] - place[1] * a[0],
    ]
    feature_ref[...] = jnp.zeros_like(feature_ref)
    for k in range(6):
        parts = split3(features[k])
        for j in range(3):
            row = (8 * j + k) * tiles
            feature_ref[row : row + tiles, :] = parts[j].astype(jnp.float32)

    sum_ref[...] = jnp.zeros_like(sum_ref)
    block = 32
    width = 4 if tiles % 4 == 0 else 1
    steps = tiles // width
    unroll = next(n for n in (12, 8, 6, 4, 3, 2, 1) if steps % n == 0)
    contract = (((1,), (1,)), ((), ()))

    def product(values, feature):
        highs = [value.astype(jnp.bfloat16) for value in values]
        lows = [(value - high.astype(jnp.float32)).astype(jnp.bfloat16) for value, high in zip(values, highs)]
        both = jnp.concatenate([jnp.concatenate(highs, axis=1), jnp.concatenate(lows, axis=1)], axis=0)
        return lax.dot_general(both, feature, contract, preferred_element_type=jnp.float32)

    def one(chunk):
        spans = [chunk * width + j for j in range(width)]
        feature = jnp.concatenate([feature_ref[pl.ds(tile, 32, stride=tiles), :].astype(jnp.bfloat16) for tile in spans], axis=1)
        source = [[source_ref[pl.ds(k * tiles + tile, 1), :] for k in range(3)] for tile in spans]
        for t in range(0, targets, block):
            kernels, pulls = [], []
            for j in range(width):
                sep = [column_ref[k, t : t + block, :] - source[j][k] for k in range(3)]
                squared = sep[0] * sep[0] + sep[1] * sep[1] + (sep[2] * sep[2] + sigma_sq)
                inverse = lax.rsqrt(squared)
                square = inverse * inverse
                kernel = square * inverse
                kernels.append(kernel)
                if t >= LANES:
                    along = column_ref[3, t : t + block, :] * sep[0] + column_ref[4, t : t + block, :] * sep[1] + column_ref[5, t : t + block, :] * sep[2]
                    pulls.append((kernel * square) * along)
            rows = slice(2 * t, 2 * t + 2 * block)
            sum_ref[rows, 0:32] = sum_ref[rows, 0:32] + product(kernels, feature)
            if t >= LANES:
                rows = slice(2 * (targets + t - LANES), 2 * (targets + t - LANES) + 2 * block)
                sum_ref[rows, 0:32] = sum_ref[rows, 0:32] + product(pulls, feature)

    def step(index, _):
        for j in range(unroll):
            one(index * unroll + j)
        return 0

    lax.fori_loop(0, steps // unroll, step, 0)

    def combined(begin, end):
        parts = [sum_ref[2 * t : 2 * t + block] + sum_ref[2 * t + block : 2 * t + 2 * block] for t in range(begin, end, block)]
        rest = -(end - begin) % LANES
        if rest:
            parts.append(jnp.zeros((rest, LANES), jnp.float32))
        turned = jnp.transpose(jnp.concatenate(parts, axis=0))
        return turned[0:8] + turned[8:16] + turned[16:24]

    found = combined(0, targets)
    pulled = combined(targets, targets + half)

    def crossed(place, rows):
        return [
            place[1] * rows[2:3] - place[2] * rows[1:2] - rows[3:4],
            place[2] * rows[0:1] - place[0] * rows[2:3] - rows[4:5],
            place[0] * rows[1:2] - place[1] * rows[0:1] - rows[5:6],
        ]

    own = own_ref[0:GROUPS, :]
    slots = target_rows(own)
    near = found[:, LANES:]
    alive = (lax.broadcasted_iota(jnp.int32, (1, LANES), 1) < live_ref[0]).astype(jnp.float32)
    blob_place = [own[k : k + 1] - centre[k] for k in range(3)]
    slot_place = [slots[k] - centre[k] for k in range(3)]
    a = slots[3:]
    first = [
        a[1] * near[2:3] - a[2] * near[1:2],
        a[2] * near[0:1] - a[0] * near[2:3],
        a[0] * near[1:2] - a[1] * near[0:1],
    ]
    blob_velocity = crossed(blob_place, found[:, 0:LANES])
    slot_velocity = crossed(slot_place, near)
    second = crossed(slot_place, pulled)
    for k in range(3):
        blob_ref[k : k + 1, :] = -kernel_scale * blob_velocity[k]
        rates_ref[k : k + 1, :] = (-kernel_scale * slot_velocity[k] * alive)[:, 0:half]
        rates_ref[3 + k : 4 + k, :] = (-kernel_scale * (first[k] - 3.0 * second[k]) * alive)[:, 0:half]


def partners(count, start):
    pairs = [(i, i + 1) for i in range(start, count - 1, 2)]
    return pairs + [(j, i) for i, j in pairs]


def per_device(positions, strengths, live_counts, vorticity, diffusivity, seed_counts):
    _, cells_x, cells_y, cells_z = vorticity.shape
    slot_count = positions.shape[1]
    y_axes = ("src", "grp")
    everyone = ("tgt", "src", "grp")
    x_count, y_count = lax.axis_size("tgt"), lax.axis_size("src") * lax.axis_size("grp")
    devices = x_count * y_count
    f32 = jnp.float32

    def kept(*shape):
        return pltpu.VMEM(shape, f32)

    def held(array):
        return pltpu.with_memory_space_constraint(array, pltpu.VMEM)

    xa, xb, ya, yb = pl.pallas_call(
        faces_kernel,
        name="faces",
        out_shape=(kept(3, cells_y, cells_z), kept(3, cells_y, cells_z), kept(3, cells_x, cells_z), kept(3, cells_x, cells_z)),
        in_specs=[pl.BlockSpec(memory_space=pl.ANY)],
        out_specs=[VMEM] * 4,
        scratch_shapes=[
            pltpu.VMEM((3, cells_x, 8, cells_z), f32),
            pltpu.VMEM((3, cells_x, 8, cells_z), f32),
            pltpu.SemaphoreType.DMA((4,)),
        ],
    )(vorticity)
    xa = held(lax.ppermute(xa, "tgt", partners(x_count, 0)))
    xb = held(lax.ppermute(xb, "tgt", partners(x_count, 1)))
    ya = held(lax.ppermute(ya, y_axes, partners(y_count, 0)))
    yb = held(lax.ppermute(yb, y_axes, partners(y_count, 1)))

    v, d, c = held(vorticity), diffusivity, seed_counts
    sums, wx, wy, rows = pl.pallas_call(
        local_kernel,
        name="local",
        out_shape=(kept(8, cells_z), kept(2, cells_y, cells_z), kept(2, cells_x, cells_z), kept(8, LANES)),
        in_specs=[SMEM] + [VMEM] * 5,
        out_specs=[VMEM] * 4,
    )(live_counts, v, d, c, positions, strengths)
    block, own = pl.pallas_call(
        block_kernel,
        name="block",
        out_shape=(jax.ShapeDtypeStruct((devices * GROUPS, LANES), f32), kept(16, LANES)),
        in_specs=[VMEM] * 8,
        out_specs=[VMEM] * 2,
    )(held(sums), held(wx), held(wy), held(rows), xa, xb, ya, yb)
    everything = lax.all_to_all(block.reshape(-1), everyone, 0, 0, tiled=True).reshape(devices * GROUPS, LANES)

    targets = LANES + slot_count
    vorticity_next, columns = pl.pallas_call(
        grid_kernel,
        name="grid",
        out_shape=(jax.ShapeDtypeStruct(vorticity.shape, f32), kept(6, targets, LANES)),
        in_specs=[VMEM] * 7,
        out_specs=[VMEM] * 2,
    )(v, d, xa, xb, ya, yb, held(own))

    tiles = devices + devices // 2
    particle_rates, blob_velocity = pl.pallas_call(
        functools.partial(pair_kernel, cells=(cells_x, cells_y, cells_z)),
        name="pairs",
        out_shape=(jax.ShapeDtypeStruct((6, slot_count), f32), jax.ShapeDtypeStruct((3, LANES), f32)),
        in_specs=[SMEM] + [VMEM] * 3,
        out_specs=[VMEM, VMEM],
        scratch_shapes=[
            pltpu.VMEM((3 * tiles, LANES), f32),
            pltpu.VMEM((32 * tiles, LANES), f32),
            pltpu.VMEM((devices, LANES), f32),
            pltpu.VMEM((2 * targets + 2 * slot_count, LANES), f32),
        ],
    )(live_counts, held(everything), held(own), held(columns))
    return (vorticity_next, particle_rates, blob_velocity)


def solution(mesh):
    placed = (
        P(None, ("tgt", "src", "grp")),
        P(None, ("tgt", "src", "grp")),
        P(("tgt", "src", "grp")),
        P(None, "tgt", ("src", "grp"), None),
        P("tgt", ("src", "grp"), None),
        P("tgt", ("src", "grp"), None),
    )
    return jax.shard_map(
        per_device,
        mesh=mesh,
        in_specs=placed,
        out_specs=(
            P(None, "tgt", ("src", "grp"), None),
            P(None, ("tgt", "src", "grp")),
            P(None, ("tgt", "src", "grp")),
        ),
        check_vma=False,
    )
```

```python
import functools
import jax
import jax.numpy as jnp
from jax import lax
from jax.experimental import pallas as pl
from jax.experimental.pallas import tpu as pltpu
from jax.sharding import PartitionSpec as P

BZ = 2
LANES = 128
GROUPS = 9

sigma_sq = 0.0004
kernel_scale = 0.25 / 3.141592653589793
seed_weight = 0.0001


VMEM = pl.BlockSpec(memory_space=pltpu.VMEM)


def split3(value):
    high = value.astype(jnp.bfloat16)
    rest = value - high.astype(jnp.float32)
    middle = rest.astype(jnp.bfloat16)
    low = (rest - middle.astype(jnp.float32)).astype(jnp.bfloat16)
    return high, middle, low


def pair_lanes(rows):
    length = rows.shape[1]
    cell = lax.broadcasted_iota(jnp.int32, (length, length // BZ), 0)
    blob = lax.broadcasted_iota(jnp.int32, (length, length // BZ), 1)
    chosen = jnp.where((cell >= blob * BZ) & (cell < blob * BZ + BZ), 1.0, 0.0).astype(jnp.bfloat16)
    total = None
    for part in split3(rows):
        product = jnp.dot(part, chosen, preferred_element_type=jnp.float32)
        total = product if total is None else total + product
    return total


def shifted_rows(value, step):
    rows = lax.broadcasted_iota(jnp.int32, value.shape, 0)
    count = value.shape[0]
    if step == 1:
        return jnp.where(rows == 0, 0.0, pltpu.roll(value, 1, 0))
    return jnp.where(rows == count - 1, 0.0, pltpu.roll(value, count - 1, 0))


def shifted_lanes(value, step):
    lanes = lax.broadcasted_iota(jnp.int32, value.shape, 1)
    count = value.shape[1]
    if step == 1:
        return jnp.where(lanes == 0, 0.0, pltpu.roll(value, 1, 1))
    return jnp.where(lanes == count - 1, 0.0, pltpu.roll(value, count - 1, 1))


def here():
    x_index = lax.axis_index("tgt")
    y_index = lax.axis_index("src") * lax.axis_size("grp") + lax.axis_index("grp")
    return x_index, y_index


def middle(cells):
    x_index, y_index = here()
    return [
        (x_index.astype(jnp.float32) + 0.5) * (cells[0] / cells[2]),
        (y_index.astype(jnp.float32) + 0.5) * (cells[1] / cells[2]),
        0.5,
    ]


def faces_kernel(v_ref, xa_ref, xb_ref, ya_ref, yb_ref, low_ref, high_ref, sems):
    _, cells_x, cells_y, _ = v_ref.shape
    x_index, y_index = here()
    x_even = lax.rem(x_index, 2) == 0
    y_even = lax.rem(y_index, 2) == 0
    top = (cells_y - 1) // 8 * 8
    last = cells_x - 1
    copies = [
        pltpu.make_async_copy(v_ref.at[:, jnp.where(x_even, 0, last)], xb_ref, sems.at[0]),
        pltpu.make_async_copy(v_ref.at[:, jnp.where(x_even, last, 0)], xa_ref, sems.at[1]),
        pltpu.make_async_copy(v_ref.at[:, :, 0:8], low_ref, sems.at[2]),
        pltpu.make_async_copy(v_ref.at[:, :, top : top + 8], high_ref, sems.at[3]),
    ]
    for copy in copies:
        copy.start()
    copies[2].wait()
    copies[3].wait()
    for k in range(3):
        first = low_ref[k, :, 0, :]
        final = high_ref[k, :, cells_y - 1 - top, :]
        ya_ref[k] = jnp.where(y_even, final, first)
        yb_ref[k] = jnp.where(y_even, first, final)
    copies[0].wait()
    copies[1].wait()


def local_kernel(live_ref, v_ref, d_ref, c_ref, position_ref, strength_ref, sums_ref, wx_ref, wy_ref, row_ref):
    _, cells_x, cells_y, cells_z = v_ref.shape
    slot_count = position_ref.shape[1]
    w = []
    c = []
    for x in range(cells_x):
        counts = c_ref[x].astype(jnp.float32)
        c.append(counts)
        w.append(counts * d_ref[x])
    wx_ref[0] = w[0]
    wx_ref[1] = w[cells_x - 1]
    for x in range(cells_x):
        wy_ref[0, x : x + 1, :] = w[x][0:1, :]
        wy_ref[1, x : x + 1, :] = w[x][cells_y - 1 : cells_y, :]
    zero = jnp.zeros((cells_y, cells_z), jnp.float32)
    at = [zero] * 3
    after = [zero] * 3
    before = [zero] * 3
    plain = zero
    moment = zero
    for x in range(cells_x):
        beside = shifted_rows(w[x], 1) + shifted_rows(w[x], -1)
        if x > 0:
            beside = beside + w[x - 1]
        if x < cells_x - 1:
            beside = beside + w[x + 1]
        around = c[x] + (beside - 6.0 * w[x])
        up = shifted_lanes(w[x], 1)
        down = shifted_lanes(w[x], -1)
        for k in range(3):
            v = v_ref[k, x]
            at[k] = at[k] + around * v
            after[k] = after[k] + up * v
            before[k] = before[k] + down * v
        plain = plain + (c[x] + 1.0)
        moment = moment + (c[x] + 1.0) * (x + 0.5)
    rows = []
    for k in range(3):
        total = (
            jnp.sum(at[k], axis=0, keepdims=True)
            + shifted_lanes(jnp.sum(after[k], axis=0, keepdims=True), -1)
            + shifted_lanes(jnp.sum(before[k], axis=0, keepdims=True), 1)
        )
        rows.append(total)
    sums_ref[0:3, :] = jnp.concatenate(rows, axis=0)
    sums_ref[3:8, :] = jnp.zeros((5, cells_z), jnp.float32)
    y_centre = lax.broadcasted_iota(jnp.int32, (cells_y, cells_z), 0).astype(jnp.float32) + 0.5
    z_centre = lax.broadcasted_iota(jnp.int32, (1, cells_z), 1).astype(jnp.float32) + 0.5
    weight = jnp.sum(plain, axis=0, keepdims=True)
    moments = jnp.concatenate(
        [
            weight,
            jnp.sum(moment, axis=0, keepdims=True),
            jnp.sum(plain * y_centre, axis=0, keepdims=True),
            weight * z_centre,
            jnp.zeros((4, cells_z), jnp.float32),
        ],
        axis=0,
    )
    blobs = pair_lanes(moments)
    inverse = 1.0 / blobs[0:1]
    x_index, y_index = here()
    x_anchor = (x_index * cells_x).astype(jnp.float32)
    y_anchor = (y_index * cells_y).astype(jnp.float32)
    row_ref[0:1, :] = (blobs[1:2] * inverse + x_anchor) / cells_z
    row_ref[1:2, :] = (blobs[2:3] * inverse + y_anchor) / cells_z
    row_ref[2:3, :] = (blobs[3:4] * inverse) / cells_z
    alive = lax.broadcasted_iota(jnp.int32, (1, LANES), 1) < live_ref[...]
    row_ref[6:7, :] = jnp.where(alive, 1.0, 0.0)
    strength = jnp.where(alive[:, 0:slot_count], strength_ref[...], 0.0)
    parts = [position_ref[k : k + 1] for k in range(3)] + [strength[k : k + 1] for k in range(3)]
    for k in range(3):
        row_ref[3 + k : 4 + k, :] = jnp.concatenate(parts[2 * k : 2 * k + 2], axis=1)


def block_kernel(sums_ref, wx_ref, wy_ref, row_ref, xa_ref, xb_ref, ya_ref, yb_ref, out_ref, own_ref):
    x_index, y_index = here()
    x_even = lax.rem(x_index, 2) == 0
    y_even = lax.rem(y_index, 2) == 0
    total = sums_ref[...]
    rows = []
    for k in range(3):
        first = jnp.where(x_even, xb_ref[k], xa_ref[k])
        last = jnp.where(x_even, xa_ref[k], xb_ref[k])
        row = jnp.sum(wx_ref[0] * first + wx_ref[1] * last, axis=0, keepdims=True)
        first = jnp.where(y_even, yb_ref[k], ya_ref[k])
        last = jnp.where(y_even, ya_ref[k], yb_ref[k])
        row = row + jnp.sum(wy_ref[0] * first + wy_ref[1] * last, axis=0, keepdims=True)
        rows.append(row)
    total = total + jnp.concatenate(rows + [jnp.zeros((5, total.shape[1]), jnp.float32)], axis=0)
    strength = seed_weight * pair_lanes(total)
    block = jnp.concatenate([row_ref[0:3], strength[0:3], row_ref[3:6]], axis=0)
    own_ref[0:GROUPS, :] = block
    own_ref[GROUPS : GROUPS + 1, :] = row_ref[6:7, :]
    devices = out_ref.shape[0] // GROUPS
    for device in range(devices):
        out_ref[device * GROUPS : (device + 1) * GROUPS, :] = block


def target_rows(own):
    rows = []
    for k in range(3):
        row = own[6 + k : 7 + k]
        rows.append(row)
        rows.append(pltpu.roll(row, LANES // 2, 1))
    return rows


def grid_kernel(v_ref, d_ref, xa_ref, xb_ref, ya_ref, yb_ref, own_ref, out_ref, column_ref, factor_ref):
    _, cells_x, cells_y, cells_z = v_ref.shape
    x_index, y_index = here()
    x_even = lax.rem(x_index, 2) == 0
    y_even = lax.rem(y_index, 2) == 0
    rows = lax.broadcasted_iota(jnp.int32, (cells_y, cells_z), 0)
    for k in range(3):
        before = jnp.where(x_even, xb_ref[k], xa_ref[k])
        beyond = jnp.where(x_even, xa_ref[k], xb_ref[k])
        first = jnp.where(y_even, yb_ref[k], ya_ref[k])
        last = jnp.where(y_even, ya_ref[k], yb_ref[k])
        for x in range(cells_x):
            v = v_ref[k, x]
            low = before if x == 0 else v_ref[k, x - 1]
            high = beyond if x == cells_x - 1 else v_ref[k, x + 1]
            left = jnp.where(rows == 0, first[x : x + 1], pltpu.roll(v, 1, 0))
            right = jnp.where(rows == cells_y - 1, last[x : x + 1], pltpu.roll(v, cells_y - 1, 0))
            beside = (high + low) + (right + left) + (shifted_lanes(v, -1) + shifted_lanes(v, 1))
            out_ref[k, x] = v + d_ref[x] * (beside - 6.0 * v)

    own = own_ref[0:GROUPS, :]
    centre = middle((cells_x, cells_y, cells_z))
    particles = target_rows(own)
    zeros = jnp.zeros((1, LANES), jnp.float32)
    place = [own[k : k + 1] - centre[k] for k in range(2)]
    slot_place = [particles[k] - centre[k] for k in range(3)]
    a = particles[3:]
    along = a[0] * slot_place[0] + a[1] * slot_place[1] + a[2] * slot_place[2]
    factors = [
        jnp.concatenate([-2.0 * place[0], -a[0]], axis=1),
        jnp.concatenate([-2.0 * place[1], -a[1]], axis=1),
        jnp.concatenate([zeros, -a[2]], axis=1),
        jnp.concatenate([place[0] * place[0] + place[1] * place[1], along], axis=1),
    ]
    factors = [[part.astype(jnp.float32) for part in split3(factor)] for factor in factors]
    nothing = jnp.zeros((1, 2 * LANES), jnp.float32)
    ones = jnp.concatenate([zeros + 1.0, zeros], axis=1)
    table = []
    for j in range(3):
        for k in range(3):
            table += [factors[k][j]] * 3
        table += [ones if j == 0 else nothing] * 3
        table += [factors[3][j]] + [nothing] * 3
    table += [jnp.concatenate([own[k : k + 1], particles[k]], axis=1) for k in range(3)]
    table += [nothing] * (LANES - len(table))
    columns = jnp.transpose(jnp.concatenate(table, axis=0))
    targets = column_ref.shape[1]
    factor_ref[...] = columns[0:targets].astype(jnp.bfloat16)
    for k in range(3):
        begin = LANES if k < 2 else 0
        column_ref[k, begin:targets, :] = jnp.broadcast_to(columns[begin:targets, 48 + k : 49 + k], (targets - begin, LANES))


def pair_kernel(all_ref, own_ref, column_ref, factor_ref, rates_ref, blob_ref, source_ref, coordinate_ref, feature_ref, turn_ref, flat_ref, sum_ref, *, cells):
    devices = all_ref.shape[0] // GROUPS
    half = LANES // 2
    tiles = devices + devices // 2
    targets = column_ref.shape[1]
    lane = lax.broadcasted_iota(jnp.int32, (devices, LANES), 1)
    centre = middle(cells)

    def group(index):
        return all_ref[pl.ds(index, devices, stride=GROUPS), :]

    def evens(rows):
        turn_ref[...] = rows
        return turn_ref[pl.ds(0, devices // 2, stride=2), :]

    blobs = [group(k) for k in range(6)]
    particles = []
    for k in range(3):
        both = group(6 + k)
        turned = pltpu.roll(both, half, 1)
        particles.append(evens(jnp.where(lane < half, both, pltpu.roll(turned, devices - 1, 0))))
        particles.append(evens(jnp.where(lane < half, turned, pltpu.roll(both, devices - 1, 0))))
    elements = [jnp.concatenate([blobs[k], particles[k]], axis=0) for k in range(6)]
    for k in range(3):
        source_ref[k * tiles : (k + 1) * tiles, :] = elements[k]
    place = [elements[k] - centre[k] for k in range(3)]
    a = elements[3:]
    features = a + [
        place[1] * a[2] - place[2] * a[1],
        place[2] * a[0] - place[0] * a[2],
        place[0] * a[1] - place[1] * a[0],
    ]
    feature_ref[...] = jnp.zeros_like(feature_ref)
    for k in range(6):
        parts = split3(features[k])
        for j in range(3):
            row = (8 * j + k) * tiles
            feature_ref[row : row + tiles, :] = parts[j].astype(jnp.float32)

    flat = place[0] * place[0] + place[1] * place[1] + sigma_sq
    for k, value in enumerate(place + [flat]):
        parts = split3(value)
        for j in range(3):
            row = (3 * k + j) * tiles
            coordinate_ref[row : row + tiles, :] = parts[j].astype(jnp.float32)
    coordinate_ref[12 * tiles : 13 * tiles, :] = jnp.ones((tiles, LANES), jnp.float32)
    coordinate_ref[13 * tiles :, :] = jnp.zeros((3 * tiles, LANES), jnp.float32)

    sum_ref[...] = jnp.zeros_like(sum_ref)
    factors = factor_ref[:, 0:48]
    block = half
    width = 4 if tiles % 4 == 0 else 1
    steps = tiles // width
    unroll = next(n for n in (12, 8, 6, 4, 2, steps) if steps % n == 0 and (n % 2 == 0 or n == steps))
    contract = (((1,), (1,)), ((), ()))

    def product(values, feature):
        highs = [value.astype(jnp.bfloat16) for value in values]
        lows = [(value - high.astype(jnp.float32)).astype(jnp.bfloat16) for value, high in zip(values, highs)]
        both = jnp.concatenate([jnp.concatenate(highs, axis=1), jnp.concatenate(lows, axis=1)], axis=0)
        return lax.dot_general(feature, both, contract, preferred_element_type=jnp.float32)

    def ahead(chunk, slot):
        spans = [chunk * width + j for j in range(width)]
        coordinate = jnp.concatenate([coordinate_ref[pl.ds(tile, 16, stride=tiles), :].astype(jnp.bfloat16) for tile in spans], axis=1)
        flat_ref[slot] = jnp.dot(factors, jnp.concatenate([coordinate] * 3, axis=0), preferred_element_type=jnp.float32)

    def one(chunk, slot):
        spans = [chunk * width + j for j in range(width)]
        feature = jnp.concatenate([feature_ref[pl.ds(tile, 32, stride=tiles), :].astype(jnp.bfloat16) for tile in spans], axis=1)
        ahead(jnp.minimum(chunk + 1, steps - 1), 1 - slot)
        source = [[source_ref[pl.ds(k * tiles + tile, 1), :] for k in range(3)] for tile in spans]
        for t in range(0, targets, block):
            kernels, pulls = [], []
            for j in range(width):
                known = flat_ref[slot, t : t + block, j * LANES : (j + 1) * LANES]
                deep = column_ref[2, t : t + block, :] - source[j][2]
                if t < LANES:
                    squared = deep * deep + known
                else:
                    sep = [column_ref[k, t : t + block, :] - source[j][k] for k in range(2)]
                    squared = sep[0] * sep[0] + sep[1] * sep[1] + (deep * deep + sigma_sq)
                inverse = lax.rsqrt(squared)
                square = inverse * inverse
                kernel = square * inverse
                kernels.append(kernel)
                if t >= LANES:
                    pulls.append((kernel * square) * known)
            sum_ref[t // block] = sum_ref[t // block] + product(kernels, feature)
            if t >= LANES:
                sum_ref[3] = sum_ref[3] + product(pulls, feature)

    def step(index, _):
        for j in range(unroll):
            one(index * unroll + j, j % 2)
        return 0

    ahead(0, 0)
    lax.fori_loop(0, steps // unroll, step, 0)

    def combined(index):
        parts = sum_ref[index, 0:8] + sum_ref[index, 8:16] + sum_ref[index, 16:24]
        return parts + pltpu.roll(parts, block, 1)

    lane = lax.broadcasted_iota(jnp.int32, (8, LANES), 1)
    found = jnp.where(lane < block, combined(0), combined(1))
    near = combined(2)
    pulled = combined(3)

    def crossed(place, rows):
        return [
            place[1] * rows[2:3] - place[2] * rows[1:2] - rows[3:4],
            place[2] * rows[0:1] - place[0] * rows[2:3] - rows[4:5],
            place[0] * rows[1:2] - place[1] * rows[0:1] - rows[5:6],
        ]

    own = own_ref[0:GROUPS, :]
    slots = target_rows(own)
    alive = own_ref[GROUPS : GROUPS + 1, :]
    blob_place = [own[k : k + 1] - centre[k] for k in range(3)]
    slot_place = [slots[k] - centre[k] for k in range(3)]
    a = slots[3:]
    first = [
        a[1] * near[2:3] - a[2] * near[1:2],
        a[2] * near[0:1] - a[0] * near[2:3],
        a[0] * near[1:2] - a[1] * near[0:1],
    ]
    blob_velocity = crossed(blob_place, found)
    slot_velocity = crossed(slot_place, near)
    second = crossed(slot_place, pulled)
    for k in range(3):
        blob_ref[k : k + 1, :] = -kernel_scale * blob_velocity[k]
        rates_ref[k : k + 1, :] = (-kernel_scale * slot_velocity[k] * alive)[:, 0:half]
        rates_ref[3 + k : 4 + k, :] = (-kernel_scale * (first[k] - 3.0 * second[k]) * alive)[:, 0:half]


def partners(count, start):
    pairs = [(i, i + 1) for i in range(start, count - 1, 2)]
    return pairs + [(j, i) for i, j in pairs]


def per_device(positions, strengths, live_counts, vorticity, diffusivity, seed_counts):
    _, cells_x, cells_y, cells_z = vorticity.shape
    slot_count = positions.shape[1]
    y_axes = ("src", "grp")
    everyone = ("tgt", "src", "grp")
    x_count, y_count = lax.axis_size("tgt"), lax.axis_size("src") * lax.axis_size("grp")
    devices = x_count * y_count
    f32 = jnp.float32

    def kept(*shape):
        return pltpu.VMEM(shape, f32)

    def held(array):
        return pltpu.with_memory_space_constraint(array, pltpu.VMEM)

    xa, xb, ya, yb = pl.pallas_call(
        faces_kernel,
        name="faces",
        out_shape=(kept(3, cells_y, cells_z), kept(3, cells_y, cells_z), kept(3, cells_x, cells_z), kept(3, cells_x, cells_z)),
        in_specs=[pl.BlockSpec(memory_space=pl.ANY)],
        out_specs=[VMEM] * 4,
        scratch_shapes=[
            pltpu.VMEM((3, cells_x, 8, cells_z), f32),
            pltpu.VMEM((3, cells_x, 8, cells_z), f32),
            pltpu.SemaphoreType.DMA((4,)),
        ],
    )(vorticity)
    xa = held(lax.ppermute(xa, "tgt", partners(x_count, 0)))
    xb = held(lax.ppermute(xb, "tgt", partners(x_count, 1)))
    ya = held(lax.ppermute(ya, y_axes, partners(y_count, 0)))
    yb = held(lax.ppermute(yb, y_axes, partners(y_count, 1)))

    v, d, c = held(vorticity), diffusivity, seed_counts
    sums, wx, wy, rows = pl.pallas_call(
        local_kernel,
        name="local",
        out_shape=(kept(8, cells_z), kept(2, cells_y, cells_z), kept(2, cells_x, cells_z), kept(8, LANES)),
        in_specs=[VMEM] * 6,
        out_specs=[VMEM] * 4,
    )(live_counts.reshape(1, 1), v, d, c, positions, strengths)
    block, own = pl.pallas_call(
        block_kernel,
        name="block",
        out_shape=(jax.ShapeDtypeStruct((devices * GROUPS, LANES), f32), kept(16, LANES)),
        in_specs=[VMEM] * 8,
        out_specs=[VMEM] * 2,
    )(held(sums), held(wx), held(wy), held(rows), xa, xb, ya, yb)
    everything = lax.all_to_all(block.reshape(-1), everyone, 0, 0, tiled=True).reshape(devices * GROUPS, LANES)

    targets = LANES + slot_count
    vorticity_next, columns, factors = pl.pallas_call(
        grid_kernel,
        name="grid",
        out_shape=(jax.ShapeDtypeStruct(vorticity.shape, f32), kept(3, targets, LANES), pltpu.VMEM((targets, LANES), jnp.bfloat16)),
        in_specs=[VMEM] * 7,
        out_specs=[VMEM] * 3,
    )(v, d, xa, xb, ya, yb, held(own))

    tiles = devices + devices // 2
    particle_rates, blob_velocity = pl.pallas_call(
        functools.partial(pair_kernel, cells=(cells_x, cells_y, cells_z)),
        name="pairs",
        out_shape=(jax.ShapeDtypeStruct((6, slot_count), f32), jax.ShapeDtypeStruct((3, LANES), f32)),
        in_specs=[VMEM] * 4,
        out_specs=[VMEM, VMEM],
        scratch_shapes=[
            pltpu.VMEM((3 * tiles, LANES), f32),
            pltpu.VMEM((16 * tiles, LANES), f32),
            pltpu.VMEM((32 * tiles, LANES), f32),
            pltpu.VMEM((devices, LANES), f32),
            pltpu.VMEM((2, targets, 4 * LANES), f32),
            pltpu.VMEM((4, 32, LANES), f32),
        ],
    )(held(everything), held(own), held(columns), held(factors))
    return (vorticity_next, particle_rates, blob_velocity)


def solution(mesh):
    placed = (
        P(None, ("tgt", "src", "grp")),
        P(None, ("tgt", "src", "grp")),
        P(("tgt", "src", "grp")),
        P(None, "tgt", ("src", "grp"), None),
        P("tgt", ("src", "grp"), None),
        P("tgt", ("src", "grp"), None),
    )
    return jax.shard_map(
        per_device,
        mesh=mesh,
        in_specs=placed,
        out_specs=(
            P(None, "tgt", ("src", "grp"), None),
            P(None, ("tgt", "src", "grp")),
            P(None, ("tgt", "src", "grp")),
        ),
        check_vma=False,
    )
```

```python
import functools
import jax
import jax.numpy as jnp
from jax import lax
from jax.experimental import pallas as pl
from jax.experimental.pallas import tpu as pltpu
from jax.sharding import PartitionSpec as P

BZ = 2
LANES = 128
GROUPS = 9

sigma_sq = 0.0004
kernel_scale = 0.25 / 3.141592653589793
seed_weight = 0.0001


VMEM = pl.BlockSpec(memory_space=pltpu.VMEM)


def split3(value):
    high = value.astype(jnp.bfloat16)
    rest = value - high.astype(jnp.float32)
    middle = rest.astype(jnp.bfloat16)
    low = (rest - middle.astype(jnp.float32)).astype(jnp.bfloat16)
    return high, middle, low


def pair_lanes(rows):
    length = rows.shape[1]
    cell = lax.broadcasted_iota(jnp.int32, (length, length // BZ), 0)
    blob = lax.broadcasted_iota(jnp.int32, (length, length // BZ), 1)
    chosen = jnp.where((cell >= blob * BZ) & (cell < blob * BZ + BZ), 1.0, 0.0).astype(jnp.bfloat16)
    total = None
    for part in split3(rows):
        product = jnp.dot(part, chosen, preferred_element_type=jnp.float32)
        total = product if total is None else total + product
    return total


def shifted_rows(value, step):
    rows = lax.broadcasted_iota(jnp.int32, value.shape, 0)
    count = value.shape[0]
    if step == 1:
        return jnp.where(rows == 0, 0.0, pltpu.roll(value, 1, 0))
    return jnp.where(rows == count - 1, 0.0, pltpu.roll(value, count - 1, 0))


def shifted_lanes(value, step):
    lanes = lax.broadcasted_iota(jnp.int32, value.shape, 1)
    count = value.shape[1]
    if step == 1:
        return jnp.where(lanes == 0, 0.0, pltpu.roll(value, 1, 1))
    return jnp.where(lanes == count - 1, 0.0, pltpu.roll(value, count - 1, 1))


def here():
    x_index = lax.axis_index("tgt")
    y_index = lax.axis_index("src") * lax.axis_size("grp") + lax.axis_index("grp")
    return x_index, y_index


def middle(cells):
    x_index, y_index = here()
    return [
        (x_index.astype(jnp.float32) + 0.5) * (cells[0] / cells[2]),
        (y_index.astype(jnp.float32) + 0.5) * (cells[1] / cells[2]),
        0.5,
    ]


def faces_kernel(v_ref, xa_ref, xb_ref, ya_ref, yb_ref, low_ref, high_ref, sems):
    _, cells_x, cells_y, _ = v_ref.shape
    x_index, y_index = here()
    x_even = lax.rem(x_index, 2) == 0
    y_even = lax.rem(y_index, 2) == 0
    last = cells_x - 1
    copies = [
        pltpu.make_async_copy(v_ref.at[:, jnp.where(x_even, 0, last)], xb_ref, sems.at[0]),
        pltpu.make_async_copy(v_ref.at[:, jnp.where(x_even, last, 0)], xa_ref, sems.at[1]),
        pltpu.make_async_copy(v_ref.at[:, :, 0:1], low_ref, sems.at[2]),
        pltpu.make_async_copy(v_ref.at[:, :, cells_y - 1 : cells_y], high_ref, sems.at[3]),
    ]
    for copy in copies[2:] + copies[:2]:
        copy.start()
    copies[2].wait()
    copies[3].wait()
    for k in range(3):
        first = low_ref[k, :, 0, :]
        final = high_ref[k, :, 0, :]
        ya_ref[k] = jnp.where(y_even, final, first)
        yb_ref[k] = jnp.where(y_even, first, final)
    copies[0].wait()
    copies[1].wait()


def local_kernel(live_ref, v_ref, d_ref, c_ref, position_ref, strength_ref, sums_ref, wx_ref, wy_ref, row_ref):
    _, cells_x, cells_y, cells_z = v_ref.shape
    slot_count = position_ref.shape[1]
    w = []
    c = []
    for x in range(cells_x):
        counts = c_ref[x].astype(jnp.float32)
        c.append(counts)
        w.append(counts * d_ref[x])
    wx_ref[0] = w[0]
    wx_ref[1] = w[cells_x - 1]
    for x in range(cells_x):
        wy_ref[0, x : x + 1, :] = w[x][0:1, :]
        wy_ref[1, x : x + 1, :] = w[x][cells_y - 1 : cells_y, :]
    zero = jnp.zeros((cells_y, cells_z), jnp.float32)
    at = [zero] * 3
    after = [zero] * 3
    before = [zero] * 3
    plain = zero
    moment = zero
    for x in range(cells_x):
        beside = shifted_rows(w[x], 1) + shifted_rows(w[x], -1)
        if x > 0:
            beside = beside + w[x - 1]
        if x < cells_x - 1:
            beside = beside + w[x + 1]
        around = c[x] + (beside - 6.0 * w[x])
        up = shifted_lanes(w[x], 1)
        down = shifted_lanes(w[x], -1)
        for k in range(3):
            v = v_ref[k, x]
            at[k] = at[k] + around * v
            after[k] = after[k] + up * v
            before[k] = before[k] + down * v
        plain = plain + (c[x] + 1.0)
        moment = moment + (c[x] + 1.0) * (x + 0.5)
    rows = []
    for k in range(3):
        total = (
            jnp.sum(at[k], axis=0, keepdims=True)
            + shifted_lanes(jnp.sum(after[k], axis=0, keepdims=True), -1)
            + shifted_lanes(jnp.sum(before[k], axis=0, keepdims=True), 1)
        )
        rows.append(total)
    sums_ref[0:3, :] = jnp.concatenate(rows, axis=0)
    sums_ref[3:8, :] = jnp.zeros((5, cells_z), jnp.float32)
    y_centre = lax.broadcasted_iota(jnp.int32, (cells_y, cells_z), 0).astype(jnp.float32) + 0.5
    z_centre = lax.broadcasted_iota(jnp.int32, (1, cells_z), 1).astype(jnp.float32) + 0.5
    weight = jnp.sum(plain, axis=0, keepdims=True)
    moments = jnp.concatenate(
        [
            weight,
            jnp.sum(moment, axis=0, keepdims=True),
            jnp.sum(plain * y_centre, axis=0, keepdims=True),
            weight * z_centre,
            jnp.zeros((4, cells_z), jnp.float32),
        ],
        axis=0,
    )
    blobs = pair_lanes(moments)
    inverse = 1.0 / blobs[0:1]
    x_index, y_index = here()
    x_anchor = (x_index * cells_x).astype(jnp.float32)
    y_anchor = (y_index * cells_y).astype(jnp.float32)
    row_ref[0:1, :] = (blobs[1:2] * inverse + x_anchor) / cells_z
    row_ref[1:2, :] = (blobs[2:3] * inverse + y_anchor) / cells_z
    row_ref[2:3, :] = (blobs[3:4] * inverse) / cells_z
    alive = lax.broadcasted_iota(jnp.int32, (1, LANES), 1) < live_ref[...]
    row_ref[6:7, :] = jnp.where(alive, 1.0, 0.0)
    strength = jnp.where(alive[:, 0:slot_count], strength_ref[...], 0.0)
    parts = [position_ref[k : k + 1] for k in range(3)] + [strength[k : k + 1] for k in range(3)]
    for k in range(3):
        row_ref[3 + k : 4 + k, :] = jnp.concatenate(parts[2 * k : 2 * k + 2], axis=1)


def block_kernel(sums_ref, wx_ref, wy_ref, row_ref, xa_ref, xb_ref, ya_ref, yb_ref, out_ref, own_ref):
    x_index, y_index = here()
    x_even = lax.rem(x_index, 2) == 0
    y_even = lax.rem(y_index, 2) == 0
    total = sums_ref[...]
    rows = []
    for k in range(3):
        first = jnp.where(x_even, xb_ref[k], xa_ref[k])
        last = jnp.where(x_even, xa_ref[k], xb_ref[k])
        row = jnp.sum(wx_ref[0] * first + wx_ref[1] * last, axis=0, keepdims=True)
        first = jnp.where(y_even, yb_ref[k], ya_ref[k])
        last = jnp.where(y_even, ya_ref[k], yb_ref[k])
        row = row + jnp.sum(wy_ref[0] * first + wy_ref[1] * last, axis=0, keepdims=True)
        rows.append(row)
    total = total + jnp.concatenate(rows + [jnp.zeros((5, total.shape[1]), jnp.float32)], axis=0)
    strength = seed_weight * pair_lanes(total)
    block = jnp.concatenate([row_ref[0:3], strength[0:3], row_ref[3:6]], axis=0)
    own_ref[0:GROUPS, :] = block
    own_ref[GROUPS : GROUPS + 1, :] = row_ref[6:7, :]
    devices = out_ref.shape[0] // GROUPS
    for device in range(devices):
        out_ref[device * GROUPS : (device + 1) * GROUPS, :] = block


def target_rows(own):
    rows = []
    for k in range(3):
        row = own[6 + k : 7 + k]
        rows.append(row)
        rows.append(pltpu.roll(row, LANES // 2, 1))
    return rows


def grid_kernel(v_ref, d_ref, xa_ref, xb_ref, ya_ref, yb_ref, own_ref, out_ref, column_ref, factor_ref):
    _, cells_x, cells_y, cells_z = v_ref.shape
    x_index, y_index = here()
    x_even = lax.rem(x_index, 2) == 0
    y_even = lax.rem(y_index, 2) == 0
    rows = lax.broadcasted_iota(jnp.int32, (cells_y, cells_z), 0)
    for k in range(3):
        before = jnp.where(x_even, xb_ref[k], xa_ref[k])
        beyond = jnp.where(x_even, xa_ref[k], xb_ref[k])
        first = jnp.where(y_even, yb_ref[k], ya_ref[k])
        last = jnp.where(y_even, ya_ref[k], yb_ref[k])
        for x in range(cells_x):
            v = v_ref[k, x]
            low = before if x == 0 else v_ref[k, x - 1]
            high = beyond if x == cells_x - 1 else v_ref[k, x + 1]
            left = jnp.where(rows == 0, first[x : x + 1], pltpu.roll(v, 1, 0))
            right = jnp.where(rows == cells_y - 1, last[x : x + 1], pltpu.roll(v, cells_y - 1, 0))
            beside = (high + low) + (right + left) + (shifted_lanes(v, -1) + shifted_lanes(v, 1))
            out_ref[k, x] = v + d_ref[x] * (beside - 6.0 * v)

    own = own_ref[0:GROUPS, :]
    centre = middle((cells_x, cells_y, cells_z))
    particles = target_rows(own)
    zeros = jnp.zeros((1, LANES), jnp.float32)
    place = [own[k : k + 1] - centre[k] for k in range(2)]
    slot_place = [particles[k] - centre[k] for k in range(3)]
    a = particles[3:]
    along = a[0] * slot_place[0] + a[1] * slot_place[1] + a[2] * slot_place[2]
    factors = [
        jnp.concatenate([-2.0 * place[0], -a[0]], axis=1),
        jnp.concatenate([-2.0 * place[1], -a[1]], axis=1),
        jnp.concatenate([zeros, -a[2]], axis=1),
        jnp.concatenate([place[0] * place[0] + place[1] * place[1], along], axis=1),
    ]
    factors = [[part.astype(jnp.float32) for part in split3(factor)] for factor in factors]
    nothing = jnp.zeros((1, 2 * LANES), jnp.float32)
    ones = jnp.concatenate([zeros + 1.0, zeros], axis=1)
    table = []
    for j in range(3):
        for k in range(3):
            table += [factors[k][j]] * 3
        table += [ones if j == 0 else nothing] * 3
        table += [factors[3][j]] + [nothing] * 3
    table += [jnp.concatenate([own[k : k + 1], particles[k]], axis=1) for k in range(3)]
    table += [nothing] * (LANES - len(table))
    columns = jnp.transpose(jnp.concatenate(table, axis=0))
    targets = column_ref.shape[1]
    factor_ref[...] = columns[0:targets].astype(jnp.bfloat16)
    for k in range(3):
        begin = LANES if k < 2 else 0
        column_ref[k, begin:targets, :] = jnp.broadcast_to(columns[begin:targets, 48 + k : 49 + k], (targets - begin, LANES))


def pair_kernel(all_ref, own_ref, column_ref, factor_ref, rates_ref, blob_ref, source_ref, coordinate_ref, feature_ref, turn_ref, flat_ref, sum_ref, *, cells):
    devices = all_ref.shape[0] // GROUPS
    half = LANES // 2
    tiles = devices + devices // 2
    targets = column_ref.shape[1]
    lane = lax.broadcasted_iota(jnp.int32, (devices, LANES), 1)
    centre = middle(cells)

    def group(index):
        return all_ref[pl.ds(index, devices, stride=GROUPS), :]

    def evens(rows):
        turn_ref[...] = rows
        return turn_ref[pl.ds(0, devices // 2, stride=2), :]

    blobs = [group(k) for k in range(6)]
    particles = []
    for k in range(3):
        both = group(6 + k)
        turned = pltpu.roll(both, half, 1)
        particles.append(evens(jnp.where(lane < half, both, pltpu.roll(turned, devices - 1, 0))))
        particles.append(evens(jnp.where(lane < half, turned, pltpu.roll(both, devices - 1, 0))))
    elements = [jnp.concatenate([blobs[k], particles[k]], axis=0) for k in range(6)]
    for k in range(3):
        source_ref[k * tiles : (k + 1) * tiles, :] = elements[k]
    place = [elements[k] - centre[k] for k in range(3)]
    a = elements[3:]
    features = a + [
        place[1] * a[2] - place[2] * a[1],
        place[2] * a[0] - place[0] * a[2],
        place[0] * a[1] - place[1] * a[0],
    ]
    feature_ref[...] = jnp.zeros_like(feature_ref)
    for k in range(6):
        parts = split3(features[k])
        for j in range(3):
            row = (8 * j + k) * tiles
            feature_ref[row : row + tiles, :] = parts[j].astype(jnp.float32)

    flat = place[0] * place[0] + place[1] * place[1] + sigma_sq
    for k, value in enumerate(place + [flat]):
        parts = split3(value)
        for j in range(3):
            row = (3 * k + j) * tiles
            coordinate_ref[row : row + tiles, :] = parts[j].astype(jnp.float32)
    coordinate_ref[12 * tiles : 13 * tiles, :] = jnp.ones((tiles, LANES), jnp.float32)
    coordinate_ref[13 * tiles :, :] = jnp.zeros((3 * tiles, LANES), jnp.float32)

    sum_ref[...] = jnp.zeros_like(sum_ref)
    factors = factor_ref[:, 0:48]
    block = half
    width = 4 if tiles % 4 == 0 else 1
    steps = tiles // width
    unroll = next(n for n in (12, 8, 6, 4, 2, steps) if steps % n == 0 and (n % 2 == 0 or n == steps))
    contract = (((1,), (1,)), ((), ()))

    def product(values, feature):
        highs = [value.astype(jnp.bfloat16) for value in values]
        lows = [(value - high.astype(jnp.float32)).astype(jnp.bfloat16) for value, high in zip(values, highs)]
        both = jnp.concatenate([jnp.concatenate(highs, axis=1), jnp.concatenate(lows, axis=1)], axis=0)
        return lax.dot_general(feature, both, contract, preferred_element_type=jnp.float32)

    def ahead(chunk, slot):
        spans = [chunk * width + j for j in range(width)]
        coordinate = jnp.concatenate([coordinate_ref[pl.ds(tile, 16, stride=tiles), :].astype(jnp.bfloat16) for tile in spans], axis=1)
        flat_ref[slot] = jnp.dot(factors, jnp.concatenate([coordinate] * 3, axis=0), preferred_element_type=jnp.float32)

    def one(chunk, slot):
        spans = [chunk * width + j for j in range(width)]
        feature = jnp.concatenate([feature_ref[pl.ds(tile, 32, stride=tiles), :].astype(jnp.bfloat16) for tile in spans], axis=1)
        ahead(jnp.minimum(chunk + 1, steps - 1), 1 - slot)
        source = [[source_ref[pl.ds(k * tiles + tile, 1), :] for k in range(3)] for tile in spans]
        for t in range(0, targets, block):
            kernels, pulls = [], []
            for j in range(width):
                known = flat_ref[slot, t : t + block, j * LANES : (j + 1) * LANES]
                deep = column_ref[2, t : t + block, :] - source[j][2]
                if t < LANES:
                    squared = deep * deep + known
                else:
                    sep = [column_ref[k, t : t + block, :] - source[j][k] for k in range(2)]
                    squared = sep[0] * sep[0] + sep[1] * sep[1] + (deep * deep + sigma_sq)
                inverse = lax.rsqrt(squared)
                square = inverse * inverse
                kernel = square * inverse
                kernels.append(kernel)
                if t >= LANES:
                    pulls.append((kernel * square) * known)
            sum_ref[t // block] = sum_ref[t // block] + product(kernels, feature)
            if t >= LANES:
                sum_ref[3] = sum_ref[3] + product(pulls, feature)

    def step(index, _):
        for j in range(unroll):
            one(index * unroll + j, j % 2)
        return 0

    ahead(0, 0)
    lax.fori_loop(0, steps // unroll, step, 0)

    def combined(index):
        parts = sum_ref[index, 0:8] + sum_ref[index, 8:16] + sum_ref[index, 16:24]
        return parts + pltpu.roll(parts, block, 1)

    lane = lax.broadcasted_iota(jnp.int32, (8, LANES), 1)
    found = jnp.where(lane < block, combined(0), combined(1))
    near = combined(2)
    pulled = combined(3)

    def crossed(place, rows):
        return [
            place[1] * rows[2:3] - place[2] * rows[1:2] - rows[3:4],
            place[2] * rows[0:1] - place[0] * rows[2:3] - rows[4:5],
            place[0] * rows[1:2] - place[1] * rows[0:1] - rows[5:6],
        ]

    own = own_ref[0:GROUPS, :]
    slots = target_rows(own)
    alive = own_ref[GROUPS : GROUPS + 1, :]
    blob_place = [own[k : k + 1] - centre[k] for k in range(3)]
    slot_place = [slots[k] - centre[k] for k in range(3)]
    a = slots[3:]
    first = [
        a[1] * near[2:3] - a[2] * near[1:2],
        a[2] * near[0:1] - a[0] * near[2:3],
        a[0] * near[1:2] - a[1] * near[0:1],
    ]
    blob_velocity = crossed(blob_place, found)
    slot_velocity = crossed(slot_place, near)
    second = crossed(slot_place, pulled)
    for k in range(3):
        blob_ref[k : k + 1, :] = -kernel_scale * blob_velocity[k]
        rates_ref[k : k + 1, :] = (-kernel_scale * slot_velocity[k] * alive)[:, 0:half]
        rates_ref[3 + k : 4 + k, :] = (-kernel_scale * (first[k] - 3.0 * second[k]) * alive)[:, 0:half]


def partners(count, start):
    pairs = [(i, i + 1) for i in range(start, count - 1, 2)]
    return pairs + [(j, i) for i, j in pairs]


def per_device(positions, strengths, live_counts, vorticity, diffusivity, seed_counts):
    _, cells_x, cells_y, cells_z = vorticity.shape
    slot_count = positions.shape[1]
    y_axes = ("src", "grp")
    everyone = ("tgt", "src", "grp")
    x_count, y_count = lax.axis_size("tgt"), lax.axis_size("src") * lax.axis_size("grp")
    devices = x_count * y_count
    f32 = jnp.float32

    def kept(*shape):
        return pltpu.VMEM(shape, f32)

    def held(array):
        return pltpu.with_memory_space_constraint(array, pltpu.VMEM)

    xa, xb, ya, yb = pl.pallas_call(
        faces_kernel,
        name="faces",
        out_shape=(kept(3, cells_y, cells_z), kept(3, cells_y, cells_z), kept(3, cells_x, cells_z), kept(3, cells_x, cells_z)),
        in_specs=[pl.BlockSpec(memory_space=pl.ANY)],
        out_specs=[VMEM] * 4,
        scratch_shapes=[
            pltpu.VMEM((3, cells_x, 1, cells_z), f32),
            pltpu.VMEM((3, cells_x, 1, cells_z), f32),
            pltpu.SemaphoreType.DMA((4,)),
        ],
    )(vorticity)
    xa = held(lax.ppermute(xa, "tgt", partners(x_count, 0)))
    xb = held(lax.ppermute(xb, "tgt", partners(x_count, 1)))
    ya = held(lax.ppermute(ya, y_axes, partners(y_count, 0)))
    yb = held(lax.ppermute(yb, y_axes, partners(y_count, 1)))

    v, d, c = vorticity, diffusivity, seed_counts
    sums, wx, wy, rows = pl.pallas_call(
        local_kernel,
        name="local",
        out_shape=(kept(8, cells_z), kept(2, cells_y, cells_z), kept(2, cells_x, cells_z), kept(8, LANES)),
        in_specs=[VMEM] * 6,
        out_specs=[VMEM] * 4,
    )(live_counts.reshape(1, 1), v, d, c, positions, strengths)
    block, own = pl.pallas_call(
        block_kernel,
        name="block",
        out_shape=(jax.ShapeDtypeStruct((devices * GROUPS, LANES), f32), kept(16, LANES)),
        in_specs=[VMEM] * 8,
        out_specs=[VMEM] * 2,
    )(held(sums), held(wx), held(wy), held(rows), xa, xb, ya, yb)
    everything = lax.all_to_all(block.reshape(-1), everyone, 0, 0, tiled=True).reshape(devices * GROUPS, LANES)

    targets = LANES + slot_count
    vorticity_next, columns, factors = pl.pallas_call(
        grid_kernel,
        name="grid",
        out_shape=(jax.ShapeDtypeStruct(vorticity.shape, f32), kept(3, targets, LANES), pltpu.VMEM((targets, LANES), jnp.bfloat16)),
        in_specs=[VMEM] * 7,
        out_specs=[VMEM] * 3,
    )(v, d, xa, xb, ya, yb, held(own))

    tiles = devices + devices // 2
    particle_rates, blob_velocity = pl.pallas_call(
        functools.partial(pair_kernel, cells=(cells_x, cells_y, cells_z)),
        name="pairs",
        out_shape=(jax.ShapeDtypeStruct((6, slot_count), f32), jax.ShapeDtypeStruct((3, LANES), f32)),
        in_specs=[VMEM] * 4,
        out_specs=[VMEM, VMEM],
        scratch_shapes=[
            pltpu.VMEM((3 * tiles, LANES), f32),
            pltpu.VMEM((16 * tiles, LANES), f32),
            pltpu.VMEM((32 * tiles, LANES), f32),
            pltpu.VMEM((devices, LANES), f32),
            pltpu.VMEM((2, targets, 4 * LANES), f32),
            pltpu.VMEM((4, 32, LANES), f32),
        ],
    )(held(everything), held(own), held(columns), held(factors))
    return (vorticity_next, particle_rates, blob_velocity)


def solution(mesh):
    placed = (
        P(None, ("tgt", "src", "grp")),
        P(None, ("tgt", "src", "grp")),
        P(("tgt", "src", "grp")),
        P(None, "tgt", ("src", "grp"), None),
        P("tgt", ("src", "grp"), None),
        P("tgt", ("src", "grp"), None),
    )
    return jax.shard_map(
        per_device,
        mesh=mesh,
        in_specs=placed,
        out_specs=(
            P(None, "tgt", ("src", "grp"), None),
            P(None, ("tgt", "src", "grp")),
            P(None, ("tgt", "src", "grp")),
        ),
        check_vma=False,
    )
```

```python
import functools
import jax
import jax.numpy as jnp
from jax import lax
from jax.experimental import pallas as pl
from jax.experimental.pallas import tpu as pltpu
from jax.sharding import PartitionSpec as P

BZ = 2
LANES = 128
GROUPS = 9

sigma_sq = 0.0004
kernel_scale = 0.25 / 3.141592653589793
seed_weight = 0.0001


VMEM = pl.BlockSpec(memory_space=pltpu.VMEM)


def split3(value):
    high = value.astype(jnp.bfloat16)
    rest = value - high.astype(jnp.float32)
    middle = rest.astype(jnp.bfloat16)
    low = (rest - middle.astype(jnp.float32)).astype(jnp.bfloat16)
    return high, middle, low


def pair_lanes(rows):
    length = rows.shape[1]
    cell = lax.broadcasted_iota(jnp.int32, (length, length // BZ), 0)
    blob = lax.broadcasted_iota(jnp.int32, (length, length // BZ), 1)
    chosen = jnp.where((cell >= blob * BZ) & (cell < blob * BZ + BZ), 1.0, 0.0).astype(jnp.bfloat16)
    total = None
    for part in split3(rows):
        product = jnp.dot(part, chosen, preferred_element_type=jnp.float32)
        total = product if total is None else total + product
    return total


def shifted_rows(value, step):
    rows = lax.broadcasted_iota(jnp.int32, value.shape, 0)
    count = value.shape[0]
    if step == 1:
        return jnp.where(rows == 0, 0.0, pltpu.roll(value, 1, 0))
    return jnp.where(rows == count - 1, 0.0, pltpu.roll(value, count - 1, 0))


def shifted_lanes(value, step):
    lanes = lax.broadcasted_iota(jnp.int32, value.shape, 1)
    count = value.shape[1]
    if step == 1:
        return jnp.where(lanes == 0, 0.0, pltpu.roll(value, 1, 1))
    return jnp.where(lanes == count - 1, 0.0, pltpu.roll(value, count - 1, 1))


def here():
    x_index = lax.axis_index("tgt")
    y_index = lax.axis_index("src") * lax.axis_size("grp") + lax.axis_index("grp")
    return x_index, y_index


def middle(cells):
    x_index, y_index = here()
    return [
        (x_index.astype(jnp.float32) + 0.5) * (cells[0] / cells[2]),
        (y_index.astype(jnp.float32) + 0.5) * (cells[1] / cells[2]),
        0.5,
    ]


def faces_kernel(v_ref, xa_ref, xb_ref, ya_ref, yb_ref, low_ref, high_ref, sems):
    _, cells_x, cells_y, _ = v_ref.shape
    x_index, y_index = here()
    x_even = lax.rem(x_index, 2) == 0
    y_even = lax.rem(y_index, 2) == 0
    last = cells_x - 1
    copies = [
        pltpu.make_async_copy(v_ref.at[:, jnp.where(x_even, 0, last)], xb_ref, sems.at[0]),
        pltpu.make_async_copy(v_ref.at[:, jnp.where(x_even, last, 0)], xa_ref, sems.at[1]),
        pltpu.make_async_copy(v_ref.at[:, :, 0:1], low_ref, sems.at[2]),
        pltpu.make_async_copy(v_ref.at[:, :, cells_y - 1 : cells_y], high_ref, sems.at[3]),
    ]
    for copy in copies[2:] + copies[:2]:
        copy.start()
    copies[2].wait()
    copies[3].wait()
    for k in range(3):
        first = low_ref[k, :, 0, :]
        final = high_ref[k, :, 0, :]
        ya_ref[k] = jnp.where(y_even, final, first)
        yb_ref[k] = jnp.where(y_even, first, final)
    copies[0].wait()
    copies[1].wait()


def local_kernel(live_ref, v_ref, d_ref, c_ref, position_ref, strength_ref, sums_ref, wx_ref, wy_ref, row_ref):
    _, cells_x, cells_y, cells_z = v_ref.shape
    slot_count = position_ref.shape[1]
    w = []
    c = []
    for x in range(cells_x):
        counts = c_ref[x].astype(jnp.float32)
        c.append(counts)
        w.append(counts * d_ref[x])
    wx_ref[0] = w[0]
    wx_ref[1] = w[cells_x - 1]
    for x in range(cells_x):
        wy_ref[0, x : x + 1, :] = w[x][0:1, :]
        wy_ref[1, x : x + 1, :] = w[x][cells_y - 1 : cells_y, :]
    zero = jnp.zeros((cells_y, cells_z), jnp.float32)
    at = [zero] * 3
    after = [zero] * 3
    before = [zero] * 3
    plain = zero
    moment = zero
    for x in range(cells_x):
        beside = shifted_rows(w[x], 1) + shifted_rows(w[x], -1)
        if x > 0:
            beside = beside + w[x - 1]
        if x < cells_x - 1:
            beside = beside + w[x + 1]
        around = c[x] + (beside - 6.0 * w[x])
        up = shifted_lanes(w[x], 1)
        down = shifted_lanes(w[x], -1)
        for k in range(3):
            v = v_ref[k, x]
            at[k] = at[k] + around * v
            after[k] = after[k] + up * v
            before[k] = before[k] + down * v
        plain = plain + (c[x] + 1.0)
        moment = moment + (c[x] + 1.0) * (x + 0.5)
    rows = []
    for k in range(3):
        total = (
            jnp.sum(at[k], axis=0, keepdims=True)
            + shifted_lanes(jnp.sum(after[k], axis=0, keepdims=True), -1)
            + shifted_lanes(jnp.sum(before[k], axis=0, keepdims=True), 1)
        )
        rows.append(total)
    sums_ref[0:3, :] = jnp.concatenate(rows, axis=0)
    sums_ref[3:8, :] = jnp.zeros((5, cells_z), jnp.float32)
    y_centre = lax.broadcasted_iota(jnp.int32, (cells_y, cells_z), 0).astype(jnp.float32) + 0.5
    z_centre = lax.broadcasted_iota(jnp.int32, (1, cells_z), 1).astype(jnp.float32) + 0.5
    weight = jnp.sum(plain, axis=0, keepdims=True)
    moments = jnp.concatenate(
        [
            weight,
            jnp.sum(moment, axis=0, keepdims=True),
            jnp.sum(plain * y_centre, axis=0, keepdims=True),
            weight * z_centre,
            jnp.zeros((4, cells_z), jnp.float32),
        ],
        axis=0,
    )
    blobs = pair_lanes(moments)
    inverse = 1.0 / blobs[0:1]
    x_index, y_index = here()
    x_anchor = (x_index * cells_x).astype(jnp.float32)
    y_anchor = (y_index * cells_y).astype(jnp.float32)
    row_ref[0:1, :] = (blobs[1:2] * inverse + x_anchor) / cells_z
    row_ref[1:2, :] = (blobs[2:3] * inverse + y_anchor) / cells_z
    row_ref[2:3, :] = (blobs[3:4] * inverse) / cells_z
    alive = lax.broadcasted_iota(jnp.int32, (1, LANES), 1) < live_ref[...]
    row_ref[6:7, :] = jnp.where(alive, 1.0, 0.0)
    strength = jnp.where(alive[:, 0:slot_count], strength_ref[...], 0.0)
    parts = [position_ref[k : k + 1] for k in range(3)] + [strength[k : k + 1] for k in range(3)]
    for k in range(3):
        row_ref[3 + k : 4 + k, :] = jnp.concatenate(parts[2 * k : 2 * k + 2], axis=1)


def block_kernel(sums_ref, wx_ref, wy_ref, row_ref, xa_ref, xb_ref, ya_ref, yb_ref, out_ref, own_ref):
    x_index, y_index = here()
    x_even = lax.rem(x_index, 2) == 0
    y_even = lax.rem(y_index, 2) == 0
    total = sums_ref[...]
    rows = []
    for k in range(3):
        first = jnp.where(x_even, xb_ref[k], xa_ref[k])
        last = jnp.where(x_even, xa_ref[k], xb_ref[k])
        row = jnp.sum(wx_ref[0] * first + wx_ref[1] * last, axis=0, keepdims=True)
        first = jnp.where(y_even, yb_ref[k], ya_ref[k])
        last = jnp.where(y_even, ya_ref[k], yb_ref[k])
        row = row + jnp.sum(wy_ref[0] * first + wy_ref[1] * last, axis=0, keepdims=True)
        rows.append(row)
    total = total + jnp.concatenate(rows + [jnp.zeros((5, total.shape[1]), jnp.float32)], axis=0)
    strength = seed_weight * pair_lanes(total)
    block = jnp.concatenate([row_ref[0:3], strength[0:3], row_ref[3:6]], axis=0)
    own_ref[0:GROUPS, :] = block
    own_ref[GROUPS : GROUPS + 1, :] = row_ref[6:7, :]
    devices = out_ref.shape[0] // GROUPS
    for device in range(devices):
        out_ref[device * GROUPS : (device + 1) * GROUPS, :] = block


def target_rows(own):
    rows = []
    for k in range(3):
        row = own[6 + k : 7 + k]
        rows.append(row)
        rows.append(pltpu.roll(row, LANES // 2, 1))
    return rows


def grid_kernel(v_ref, d_ref, xa_ref, xb_ref, ya_ref, yb_ref, own_ref, out_ref, column_ref, factor_ref):
    _, cells_x, cells_y, cells_z = v_ref.shape
    x_index, y_index = here()
    x_even = lax.rem(x_index, 2) == 0
    y_even = lax.rem(y_index, 2) == 0
    rows = lax.broadcasted_iota(jnp.int32, (cells_y, cells_z), 0)
    for k in range(3):
        before = jnp.where(x_even, xb_ref[k], xa_ref[k])
        beyond = jnp.where(x_even, xa_ref[k], xb_ref[k])
        first = jnp.where(y_even, yb_ref[k], ya_ref[k])
        last = jnp.where(y_even, ya_ref[k], yb_ref[k])
        for x in range(cells_x):
            v = v_ref[k, x]
            low = before if x == 0 else v_ref[k, x - 1]
            high = beyond if x == cells_x - 1 else v_ref[k, x + 1]
            left = jnp.where(rows == 0, first[x : x + 1], pltpu.roll(v, 1, 0))
            right = jnp.where(rows == cells_y - 1, last[x : x + 1], pltpu.roll(v, cells_y - 1, 0))
            beside = (high + low) + (right + left) + (shifted_lanes(v, -1) + shifted_lanes(v, 1))
            out_ref[k, x] = v + d_ref[x] * (beside - 6.0 * v)

    own = own_ref[0:GROUPS, :]
    centre = middle((cells_x, cells_y, cells_z))
    particles = target_rows(own)
    zeros = jnp.zeros((1, LANES), jnp.float32)
    place = [own[k : k + 1] - centre[k] for k in range(2)]
    slot_place = [particles[k] - centre[k] for k in range(3)]
    a = particles[3:]
    along = a[0] * slot_place[0] + a[1] * slot_place[1] + a[2] * slot_place[2]
    factors = [
        jnp.concatenate([-2.0 * place[0], -a[0]], axis=1),
        jnp.concatenate([-2.0 * place[1], -a[1]], axis=1),
        jnp.concatenate([zeros, -a[2]], axis=1),
        jnp.concatenate([place[0] * place[0] + place[1] * place[1], along], axis=1),
    ]
    factors = [[part.astype(jnp.float32) for part in split3(factor)] for factor in factors]
    nothing = jnp.zeros((1, 2 * LANES), jnp.float32)
    ones = jnp.concatenate([zeros + 1.0, zeros], axis=1)
    table = []
    for j in range(3):
        for k in range(3):
            table += [factors[k][j]] * 3
        table += [ones if j == 0 else nothing] * 3
        table += [factors[3][j]] + [nothing] * 3
    table += [jnp.concatenate([own[k : k + 1], particles[k]], axis=1) for k in range(3)]
    table += [nothing] * (LANES - len(table))
    columns = jnp.transpose(jnp.concatenate(table, axis=0))
    targets = column_ref.shape[1]
    factor_ref[...] = columns[0:targets].astype(jnp.bfloat16)
    for k in range(3):
        begin = LANES if k < 2 else 0
        column_ref[k, begin:targets, :] = jnp.broadcast_to(columns[begin:targets, 48 + k : 49 + k], (targets - begin, LANES))


def pair_kernel(all_ref, own_ref, column_ref, factor_ref, rates_ref, blob_ref, source_ref, coordinate_ref, feature_ref, turn_ref, flat_ref, sum_ref, *, cells):
    devices = all_ref.shape[0] // GROUPS
    half = LANES // 2
    tiles = devices + devices // 2
    pitch = tiles + 1 - tiles % 2
    lane = lax.broadcasted_iota(jnp.int32, (devices, LANES), 1)
    centre = middle(cells)

    def group(index):
        return all_ref[pl.ds(index, devices, stride=GROUPS), :]

    def evens(rows):
        turn_ref[...] = rows
        return turn_ref[pl.ds(0, devices // 2, stride=2), :]

    blobs = [group(k) for k in range(6)]
    particles = []
    for k in range(3):
        both = group(6 + k)
        turned = pltpu.roll(both, half, 1)
        particles.append(evens(jnp.where(lane < half, both, pltpu.roll(turned, devices - 1, 0))))
        particles.append(evens(jnp.where(lane < half, turned, pltpu.roll(both, devices - 1, 0))))
    elements = [jnp.concatenate([blobs[k], particles[k]], axis=0) for k in range(6)]
    for k in range(3):
        source_ref[k * tiles : (k + 1) * tiles, :] = elements[k]
    place = [elements[k] - centre[k] for k in range(3)]
    a = elements[3:]
    features = a + [
        place[1] * a[2] - place[2] * a[1],
        place[2] * a[0] - place[0] * a[2],
        place[0] * a[1] - place[1] * a[0],
    ]
    feature_ref[...] = jnp.zeros_like(feature_ref)
    for k in range(6):
        parts = split3(features[k])
        for j in range(3):
            row = (8 * j + k) * pitch
            feature_ref[row : row + tiles, :] = parts[j].astype(jnp.float32)

    flat = place[0] * place[0] + place[1] * place[1] + sigma_sq
    for k, value in enumerate(place + [flat]):
        parts = split3(value)
        for j in range(3):
            row = (3 * k + j) * pitch
            coordinate_ref[row : row + tiles, :] = parts[j].astype(jnp.float32)
    coordinate_ref[12 * pitch : 12 * pitch + tiles, :] = jnp.ones((tiles, LANES), jnp.float32)
    coordinate_ref[13 * pitch :, :] = jnp.zeros((3 * pitch, LANES), jnp.float32)

    sum_ref[...] = jnp.zeros_like(sum_ref)
    factors = factor_ref[:, 0:48]
    block = half
    width = 4 if tiles % 4 == 0 else 1
    steps = tiles // width
    unroll = next(n for n in (12, 8, 6, 4, 2, steps) if steps % n == 0 and (n % 2 == 0 or n == steps))
    contract = (((1,), (1,)), ((), ()))

    def product(upper, lower, feature):
        parts = []
        for values in (upper, lower):
            highs = [value.astype(jnp.bfloat16) for value in values]
            lows = [(value - high.astype(jnp.float32)).astype(jnp.bfloat16) for value, high in zip(values, highs)]
            parts += [jnp.concatenate(highs, axis=1), jnp.concatenate(lows, axis=1)]
        return lax.dot_general(feature, jnp.concatenate(parts, axis=0), contract, preferred_element_type=jnp.float32)

    def ahead(chunk, slot):
        spans = [chunk * width + j for j in range(width)]
        coordinate = jnp.concatenate([coordinate_ref[pl.ds(tile, 16, stride=pitch), :].astype(jnp.bfloat16) for tile in spans], axis=1)
        flat_ref[slot] = jnp.dot(factors, jnp.concatenate([coordinate] * 3, axis=0), preferred_element_type=jnp.float32)

    def one(chunk, slot):
        spans = [chunk * width + j for j in range(width)]
        feature = jnp.concatenate([feature_ref[pl.ds(tile, 32, stride=pitch), :].astype(jnp.bfloat16) for tile in spans], axis=1)
        ahead(jnp.minimum(chunk + 1, steps - 1), 1 - slot)
        source = [[source_ref[pl.ds(k * tiles + tile, 1), :] for k in range(3)] for tile in spans]
        for t in (0, LANES):
            values = [[], []]
            for j in range(width):
                for u in range(2 if t < LANES else 1):
                    row = t + u * block
                    known = flat_ref[slot, row : row + block, j * LANES : (j + 1) * LANES]
                    deep = column_ref[2, row : row + block, :] - source[j][2]
                    if t < LANES:
                        squared = deep * deep + known
                    else:
                        sep = [column_ref[k, row : row + block, :] - source[j][k] for k in range(2)]
                        squared = sep[0] * sep[0] + sep[1] * sep[1] + (deep * deep + sigma_sq)
                    inverse = lax.rsqrt(squared)
                    square = inverse * inverse
                    kernel = square * inverse
                    values[u].append(kernel)
                    if t >= LANES:
                        values[1].append((kernel * square) * known)
            sum_ref[t // LANES] = sum_ref[t // LANES] + product(values[0], values[1], feature)

    def step(index, _):
        for j in range(unroll):
            one(index * unroll + j, j % 2)
        return 0

    ahead(0, 0)
    lax.fori_loop(0, steps // unroll, step, 0)

    def combined(index):
        part = slice(index % 2 * LANES, (index % 2 + 1) * LANES)
        parts = sum_ref[index // 2, 0:8, part] + sum_ref[index // 2, 8:16, part] + sum_ref[index // 2, 16:24, part]
        return parts + pltpu.roll(parts, block, 1)

    lane = lax.broadcasted_iota(jnp.int32, (8, LANES), 1)
    found = jnp.where(lane < block, combined(0), combined(1))
    near = combined(2)
    pulled = combined(3)

    def crossed(place, rows):
        return [
            place[1] * rows[2:3] - place[2] * rows[1:2] - rows[3:4],
            place[2] * rows[0:1] - place[0] * rows[2:3] - rows[4:5],
            place[0] * rows[1:2] - place[1] * rows[0:1] - rows[5:6],
        ]

    own = own_ref[0:GROUPS, :]
    slots = target_rows(own)
    alive = own_ref[GROUPS : GROUPS + 1, :]
    blob_place = [own[k : k + 1] - centre[k] for k in range(3)]
    slot_place = [slots[k] - centre[k] for k in range(3)]
    a = slots[3:]
    first = [
        a[1] * near[2:3] - a[2] * near[1:2],
        a[2] * near[0:1] - a[0] * near[2:3],
        a[0] * near[1:2] - a[1] * near[0:1],
    ]
    blob_velocity = crossed(blob_place, found)
    slot_velocity = crossed(slot_place, near)
    second = crossed(slot_place, pulled)
    for k in range(3):
        blob_ref[k : k + 1, :] = -kernel_scale * blob_velocity[k]
        rates_ref[k : k + 1, :] = (-kernel_scale * slot_velocity[k] * alive)[:, 0:half]
        rates_ref[3 + k : 4 + k, :] = (-kernel_scale * (first[k] - 3.0 * second[k]) * alive)[:, 0:half]


def partners(count, start):
    pairs = [(i, i + 1) for i in range(start, count - 1, 2)]
    return pairs + [(j, i) for i, j in pairs]


def per_device(positions, strengths, live_counts, vorticity, diffusivity, seed_counts):
    _, cells_x, cells_y, cells_z = vorticity.shape
    slot_count = positions.shape[1]
    y_axes = ("src", "grp")
    everyone = ("tgt", "src", "grp")
    x_count, y_count = lax.axis_size("tgt"), lax.axis_size("src") * lax.axis_size("grp")
    devices = x_count * y_count
    f32 = jnp.float32

    def kept(*shape):
        return pltpu.VMEM(shape, f32)

    def held(array):
        return pltpu.with_memory_space_constraint(array, pltpu.VMEM)

    xa, xb, ya, yb = pl.pallas_call(
        faces_kernel,
        name="faces",
        out_shape=(kept(3, cells_y, cells_z), kept(3, cells_y, cells_z), kept(3, cells_x, cells_z), kept(3, cells_x, cells_z)),
        in_specs=[pl.BlockSpec(memory_space=pl.ANY)],
        out_specs=[VMEM] * 4,
        scratch_shapes=[
            pltpu.VMEM((3, cells_x, 1, cells_z), f32),
            pltpu.VMEM((3, cells_x, 1, cells_z), f32),
            pltpu.SemaphoreType.DMA((4,)),
        ],
    )(vorticity)
    xa = held(lax.ppermute(xa, "tgt", partners(x_count, 0)))
    xb = held(lax.ppermute(xb, "tgt", partners(x_count, 1)))
    ya = held(lax.ppermute(ya, y_axes, partners(y_count, 0)))
    yb = held(lax.ppermute(yb, y_axes, partners(y_count, 1)))

    v, d, c = vorticity, diffusivity, seed_counts
    sums, wx, wy, rows = pl.pallas_call(
        local_kernel,
        name="local",
        out_shape=(kept(8, cells_z), kept(2, cells_y, cells_z), kept(2, cells_x, cells_z), kept(8, LANES)),
        in_specs=[VMEM] * 6,
        out_specs=[VMEM] * 4,
    )(live_counts.reshape(1, 1), v, d, c, positions, strengths)
    block, own = pl.pallas_call(
        block_kernel,
        name="block",
        out_shape=(jax.ShapeDtypeStruct((devices * GROUPS, LANES), f32), kept(16, LANES)),
        in_specs=[VMEM] * 8,
        out_specs=[VMEM] * 2,
    )(held(sums), held(wx), held(wy), held(rows), xa, xb, ya, yb)
    everything = lax.all_to_all(block.reshape(-1), everyone, 0, 0, tiled=True).reshape(devices * GROUPS, LANES)

    targets = LANES + slot_count
    vorticity_next, columns, factors = pl.pallas_call(
        grid_kernel,
        name="grid",
        out_shape=(jax.ShapeDtypeStruct(vorticity.shape, f32), kept(3, targets, LANES), pltpu.VMEM((targets, LANES), jnp.bfloat16)),
        in_specs=[VMEM] * 7,
        out_specs=[VMEM] * 3,
    )(v, d, xa, xb, ya, yb, held(own))

    tiles = devices + devices // 2
    pitch = tiles + 1 - tiles % 2
    particle_rates, blob_velocity = pl.pallas_call(
        functools.partial(pair_kernel, cells=(cells_x, cells_y, cells_z)),
        name="pairs",
        out_shape=(jax.ShapeDtypeStruct((6, slot_count), f32), jax.ShapeDtypeStruct((3, LANES), f32)),
        in_specs=[VMEM] * 4,
        out_specs=[VMEM, VMEM],
        scratch_shapes=[
            pltpu.VMEM((3 * tiles, LANES), f32),
            pltpu.VMEM((16 * pitch, LANES), f32),
            pltpu.VMEM((32 * pitch, LANES), f32),
            pltpu.VMEM((devices, LANES), f32),
            pltpu.VMEM((2, targets, 4 * LANES), f32),
            pltpu.VMEM((2, 32, 2 * LANES), f32),
        ],
    )(held(everything), held(own), held(columns), held(factors))
    return (vorticity_next, particle_rates, blob_velocity)


def solution(mesh):
    placed = (
        P(None, ("tgt", "src", "grp")),
        P(None, ("tgt", "src", "grp")),
        P(("tgt", "src", "grp")),
        P(None, "tgt", ("src", "grp"), None),
        P("tgt", ("src", "grp"), None),
        P("tgt", ("src", "grp"), None),
    )
    return jax.shard_map(
        per_device,
        mesh=mesh,
        in_specs=placed,
        out_specs=(
            P(None, "tgt", ("src", "grp"), None),
            P(None, ("tgt", "src", "grp")),
            P(None, ("tgt", "src", "grp")),
        ),
        check_vma=False,
    )
```

```python
import functools
import jax
import jax.numpy as jnp
from jax import lax
from jax.experimental import pallas as pl
from jax.experimental.pallas import tpu as pltpu
from jax.sharding import PartitionSpec as P

BZ = 2
LANES = 128
GROUPS = 9

sigma_sq = 0.0004
kernel_scale = 0.25 / 3.141592653589793
seed_weight = 0.0001


VMEM = pl.BlockSpec(memory_space=pltpu.VMEM)


def split3(value):
    high = value.astype(jnp.bfloat16)
    rest = value - high.astype(jnp.float32)
    middle = rest.astype(jnp.bfloat16)
    low = (rest - middle.astype(jnp.float32)).astype(jnp.bfloat16)
    return high, middle, low


def pair_lanes(rows):
    length = rows.shape[1]
    cell = lax.broadcasted_iota(jnp.int32, (length, length // BZ), 0)
    blob = lax.broadcasted_iota(jnp.int32, (length, length // BZ), 1)
    chosen = jnp.where((cell >= blob * BZ) & (cell < blob * BZ + BZ), 1.0, 0.0).astype(jnp.bfloat16)
    total = None
    for part in split3(rows):
        product = jnp.dot(part, chosen, preferred_element_type=jnp.float32)
        total = product if total is None else total + product
    return total


def shifted_rows(value, step):
    rows = lax.broadcasted_iota(jnp.int32, value.shape, 0)
    count = value.shape[0]
    if step == 1:
        return jnp.where(rows == 0, 0.0, pltpu.roll(value, 1, 0))
    return jnp.where(rows == count - 1, 0.0, pltpu.roll(value, count - 1, 0))


def shifted_lanes(value, step):
    lanes = lax.broadcasted_iota(jnp.int32, value.shape, 1)
    count = value.shape[1]
    if step == 1:
        return jnp.where(lanes == 0, 0.0, pltpu.roll(value, 1, 1))
    return jnp.where(lanes == count - 1, 0.0, pltpu.roll(value, count - 1, 1))


def here():
    x_index = lax.axis_index("tgt")
    y_index = lax.axis_index("src") * lax.axis_size("grp") + lax.axis_index("grp")
    return x_index, y_index


def middle(cells):
    x_index, y_index = here()
    return [
        (x_index.astype(jnp.float32) + 0.5) * (cells[0] / cells[2]),
        (y_index.astype(jnp.float32) + 0.5) * (cells[1] / cells[2]),
        0.5,
    ]


def crossing(y_index):
    return lax.rem((y_index + 1) // 2, 2) == 1


def faces_kernel(v_ref, xb_ref, ya_ref, second_ref, third_ref, x_ref, low_ref, high_ref, sems):
    _, cells_x, cells_y, _ = v_ref.shape
    x_index, y_index = here()
    x_even = lax.rem(x_index, 2) == 0
    y_even = lax.rem(y_index, 2) == 0
    y_second = crossing(y_index)
    last = cells_x - 1
    copies = [
        pltpu.make_async_copy(v_ref.at[:, :, 0:1], low_ref, sems.at[0]),
        pltpu.make_async_copy(v_ref.at[:, :, cells_y - 1 : cells_y], high_ref, sems.at[1]),
        pltpu.make_async_copy(v_ref.at[:, jnp.where(x_even, last, 0)], x_ref, sems.at[2]),
        pltpu.make_async_copy(v_ref.at[:, jnp.where(x_even, 0, last)], xb_ref, sems.at[3]),
    ]
    for copy in copies:
        copy.start()
    for copy in copies[:3]:
        copy.wait()
    for k in range(3):
        first = low_ref[k, :, 0, :]
        final = high_ref[k, :, 0, :]
        ya_ref[k] = jnp.where(y_even, final, first)
        y_face = jnp.where(y_even, first, final)
        second_ref[k, 0:cells_y] = x_ref[k]
        third_ref[k, 0:cells_y] = x_ref[k]

        @pl.when(y_second)
        def _():
            second_ref[k, 0:cells_x] = y_face

        @pl.when(jnp.logical_not(y_second))
        def _():
            third_ref[k, 0:cells_x] = y_face

    copies[3].wait()


def layers(k, cells, xb_ref, ya_ref, second_ref, third_ref):
    cells_x, cells_y = cells
    x_index, y_index = here()
    x_even = lax.rem(x_index, 2) == 0
    y_even = lax.rem(y_index, 2) == 0
    y_second = crossing(y_index)
    xa = jnp.where(y_second, third_ref[k, 0:cells_y], second_ref[k, 0:cells_y])
    yb = jnp.where(y_second, second_ref[k, 0:cells_x], third_ref[k, 0:cells_x])
    xb, ya = xb_ref[k], ya_ref[k]
    return jnp.where(x_even, xb, xa), jnp.where(x_even, xa, xb), jnp.where(y_even, yb, ya), jnp.where(y_even, ya, yb)


def local_kernel(live_ref, v_ref, d_ref, c_ref, position_ref, strength_ref, sums_ref, wx_ref, wy_ref, row_ref):
    _, cells_x, cells_y, cells_z = v_ref.shape
    slot_count = position_ref.shape[1]
    w = []
    c = []
    for x in range(cells_x):
        counts = c_ref[x].astype(jnp.float32)
        c.append(counts)
        w.append(counts * d_ref[x])
    wx_ref[0] = w[0]
    wx_ref[1] = w[cells_x - 1]
    for x in range(cells_x):
        wy_ref[0, x : x + 1, :] = w[x][0:1, :]
        wy_ref[1, x : x + 1, :] = w[x][cells_y - 1 : cells_y, :]
    zero = jnp.zeros((cells_y, cells_z), jnp.float32)
    at = [zero] * 3
    after = [zero] * 3
    before = [zero] * 3
    plain = zero
    moment = zero
    for x in range(cells_x):
        beside = shifted_rows(w[x], 1) + shifted_rows(w[x], -1)
        if x > 0:
            beside = beside + w[x - 1]
        if x < cells_x - 1:
            beside = beside + w[x + 1]
        around = c[x] + (beside - 6.0 * w[x])
        up = shifted_lanes(w[x], 1)
        down = shifted_lanes(w[x], -1)
        for k in range(3):
            v = v_ref[k, x]
            at[k] = at[k] + around * v
            after[k] = after[k] + up * v
            before[k] = before[k] + down * v
        plain = plain + (c[x] + 1.0)
        moment = moment + (c[x] + 1.0) * (x + 0.5)
    rows = []
    for k in range(3):
        total = (
            jnp.sum(at[k], axis=0, keepdims=True)
            + shifted_lanes(jnp.sum(after[k], axis=0, keepdims=True), -1)
            + shifted_lanes(jnp.sum(before[k], axis=0, keepdims=True), 1)
        )
        rows.append(total)
    sums_ref[0:3, :] = jnp.concatenate(rows, axis=0)
    sums_ref[3:8, :] = jnp.zeros((5, cells_z), jnp.float32)
    y_centre = lax.broadcasted_iota(jnp.int32, (cells_y, cells_z), 0).astype(jnp.float32) + 0.5
    z_centre = lax.broadcasted_iota(jnp.int32, (1, cells_z), 1).astype(jnp.float32) + 0.5
    weight = jnp.sum(plain, axis=0, keepdims=True)
    moments = jnp.concatenate(
        [
            weight,
            jnp.sum(moment, axis=0, keepdims=True),
            jnp.sum(plain * y_centre, axis=0, keepdims=True),
            weight * z_centre,
            jnp.zeros((4, cells_z), jnp.float32),
        ],
        axis=0,
    )
    blobs = pair_lanes(moments)
    inverse = 1.0 / blobs[0:1]
    x_index, y_index = here()
    x_anchor = (x_index * cells_x).astype(jnp.float32)
    y_anchor = (y_index * cells_y).astype(jnp.float32)
    row_ref[0:1, :] = (blobs[1:2] * inverse + x_anchor) / cells_z
    row_ref[1:2, :] = (blobs[2:3] * inverse + y_anchor) / cells_z
    row_ref[2:3, :] = (blobs[3:4] * inverse) / cells_z
    alive = lax.broadcasted_iota(jnp.int32, (1, LANES), 1) < live_ref[...]
    row_ref[6:7, :] = jnp.where(alive, 1.0, 0.0)
    strength = jnp.where(alive[:, 0:slot_count], strength_ref[...], 0.0)
    parts = [position_ref[k : k + 1] for k in range(3)] + [strength[k : k + 1] for k in range(3)]
    for k in range(3):
        row_ref[3 + k : 4 + k, :] = jnp.concatenate(parts[2 * k : 2 * k + 2], axis=1)


def block_kernel(sums_ref, wx_ref, wy_ref, row_ref, xb_ref, ya_ref, second_ref, third_ref, out_ref, own_ref):
    total = sums_ref[...]
    cells = (wy_ref.shape[1], wx_ref.shape[1])
    rows = []
    for k in range(3):
        before, beyond, first, last = layers(k, cells, xb_ref, ya_ref, second_ref, third_ref)
        row = jnp.sum(wx_ref[0] * before + wx_ref[1] * beyond, axis=0, keepdims=True)
        rows.append(row + jnp.sum(wy_ref[0] * first + wy_ref[1] * last, axis=0, keepdims=True))
    total = total + jnp.concatenate(rows + [jnp.zeros((5, total.shape[1]), jnp.float32)], axis=0)
    strength = seed_weight * pair_lanes(total)
    block = jnp.concatenate([row_ref[0:3], strength[0:3], row_ref[3:6]], axis=0)
    own_ref[0:GROUPS, :] = block
    own_ref[GROUPS : GROUPS + 1, :] = row_ref[6:7, :]
    devices = out_ref.shape[0] // GROUPS
    for device in range(devices):
        out_ref[device * GROUPS : (device + 1) * GROUPS, :] = block


def target_rows(own):
    rows = []
    for k in range(3):
        row = own[6 + k : 7 + k]
        rows.append(row)
        rows.append(pltpu.roll(row, LANES // 2, 1))
    return rows


def grid_kernel(v_ref, d_ref, xb_ref, ya_ref, second_ref, third_ref, own_ref, out_ref, column_ref, factor_ref):
    _, cells_x, cells_y, cells_z = v_ref.shape
    rows = lax.broadcasted_iota(jnp.int32, (cells_y, cells_z), 0)
    for k in range(3):
        before, beyond, first, last = layers(k, (cells_x, cells_y), xb_ref, ya_ref, second_ref, third_ref)
        for x in range(cells_x):
            v = v_ref[k, x]
            low = before if x == 0 else v_ref[k, x - 1]
            high = beyond if x == cells_x - 1 else v_ref[k, x + 1]
            left = jnp.where(rows == 0, first[x : x + 1], pltpu.roll(v, 1, 0))
            right = jnp.where(rows == cells_y - 1, last[x : x + 1], pltpu.roll(v, cells_y - 1, 0))
            beside = (high + low) + (right + left) + (shifted_lanes(v, -1) + shifted_lanes(v, 1))
            out_ref[k, x] = v + d_ref[x] * (beside - 6.0 * v)

    own = own_ref[0:GROUPS, :]
    centre = middle((cells_x, cells_y, cells_z))
    particles = target_rows(own)
    zeros = jnp.zeros((1, LANES), jnp.float32)
    place = [own[k : k + 1] - centre[k] for k in range(2)]
    slot_place = [particles[k] - centre[k] for k in range(3)]
    a = particles[3:]
    along = a[0] * slot_place[0] + a[1] * slot_place[1] + a[2] * slot_place[2]
    factors = [
        jnp.concatenate([-2.0 * place[0], -a[0]], axis=1),
        jnp.concatenate([-2.0 * place[1], -a[1]], axis=1),
        jnp.concatenate([zeros, -a[2]], axis=1),
        jnp.concatenate([place[0] * place[0] + place[1] * place[1], along], axis=1),
    ]
    factors = [[part.astype(jnp.float32) for part in split3(factor)] for factor in factors]
    nothing = jnp.zeros((1, 2 * LANES), jnp.float32)
    ones = jnp.concatenate([zeros + 1.0, zeros], axis=1)
    table = []
    for j in range(3):
        for k in range(3):
            table += [factors[k][j]] * 3
        table += [ones if j == 0 else nothing] * 3
        table += [factors[3][j]] + [nothing] * 3
    table += [jnp.concatenate([own[k : k + 1], particles[k]], axis=1) for k in range(3)]
    table += [nothing] * (LANES - len(table))
    columns = jnp.transpose(jnp.concatenate(table, axis=0))
    targets = column_ref.shape[1]
    factor_ref[...] = columns[0:targets].astype(jnp.bfloat16)
    for k in range(3):
        begin = LANES if k < 2 else 0
        column_ref[k, begin:targets, :] = jnp.broadcast_to(columns[begin:targets, 48 + k : 49 + k], (targets - begin, LANES))


def pair_kernel(all_ref, own_ref, column_ref, factor_ref, rates_ref, blob_ref, source_ref, coordinate_ref, feature_ref, turn_ref, flat_ref, sum_ref, *, cells):
    devices = all_ref.shape[0] // GROUPS
    half = LANES // 2
    tiles = devices + devices // 2
    pitch = tiles + 1 - tiles % 2
    lane = lax.broadcasted_iota(jnp.int32, (devices, LANES), 1)
    centre = middle(cells)

    def group(index):
        return all_ref[pl.ds(index, devices, stride=GROUPS), :]

    def evens(rows):
        turn_ref[...] = rows
        return turn_ref[pl.ds(0, devices // 2, stride=2), :]

    blobs = [group(k) for k in range(6)]
    particles = []
    for k in range(3):
        both = group(6 + k)
        turned = pltpu.roll(both, half, 1)
        particles.append(evens(jnp.where(lane < half, both, pltpu.roll(turned, devices - 1, 0))))
        particles.append(evens(jnp.where(lane < half, turned, pltpu.roll(both, devices - 1, 0))))
    elements = [jnp.concatenate([blobs[k], particles[k]], axis=0) for k in range(6)]
    for k in range(3):
        source_ref[k * tiles : (k + 1) * tiles, :] = elements[k]
    place = [elements[k] - centre[k] for k in range(3)]
    a = elements[3:]
    features = a + [
        place[1] * a[2] - place[2] * a[1],
        place[2] * a[0] - place[0] * a[2],
        place[0] * a[1] - place[1] * a[0],
    ]
    feature_ref[...] = jnp.zeros_like(feature_ref)
    for k in range(6):
        parts = split3(features[k])
        for j in range(3):
            row = (8 * j + k) * pitch
            feature_ref[row : row + tiles, :] = parts[j].astype(jnp.float32)

    flat = place[0] * place[0] + place[1] * place[1] + sigma_sq
    for k, value in enumerate(place + [flat]):
        parts = split3(value)
        for j in range(3):
            row = (3 * k + j) * pitch
            coordinate_ref[row : row + tiles, :] = parts[j].astype(jnp.float32)
    coordinate_ref[12 * pitch : 12 * pitch + tiles, :] = jnp.ones((tiles, LANES), jnp.float32)
    coordinate_ref[13 * pitch :, :] = jnp.zeros((3 * pitch, LANES), jnp.float32)

    sum_ref[...] = jnp.zeros_like(sum_ref)
    factors = factor_ref[:, 0:48]
    block = half
    width = 4 if tiles % 4 == 0 else 1
    steps = tiles // width
    unroll = next(n for n in (12, 8, 6, 4, 2, steps) if steps % n == 0 and (n % 2 == 0 or n == steps))
    contract = (((1,), (1,)), ((), ()))

    def product(upper, lower, feature):
        parts = []
        for values in (upper, lower):
            highs = [value.astype(jnp.bfloat16) for value in values]
            lows = [(value - high.astype(jnp.float32)).astype(jnp.bfloat16) for value, high in zip(values, highs)]
            parts += [jnp.concatenate(highs, axis=1), jnp.concatenate(lows, axis=1)]
        return lax.dot_general(feature, jnp.concatenate(parts, axis=0), contract, preferred_element_type=jnp.float32)

    def ahead(chunk, slot):
        spans = [chunk * width + j for j in range(width)]
        coordinate = jnp.concatenate([coordinate_ref[pl.ds(tile, 16, stride=pitch), :].astype(jnp.bfloat16) for tile in spans], axis=1)
        flat_ref[slot] = jnp.dot(factors, jnp.concatenate([coordinate] * 3, axis=0), preferred_element_type=jnp.float32)

    def one(chunk, slot):
        spans = [chunk * width + j for j in range(width)]
        feature = jnp.concatenate([feature_ref[pl.ds(tile, 32, stride=pitch), :].astype(jnp.bfloat16) for tile in spans], axis=1)
        ahead(jnp.minimum(chunk + 1, steps - 1), 1 - slot)
        source = [[source_ref[pl.ds(k * tiles + tile, 1), :] for k in range(3)] for tile in spans]
        for t in (0, LANES):
            values = [[], []]
            for j in range(width):
                for u in range(2 if t < LANES else 1):
                    row = t + u * block
                    known = flat_ref[slot, row : row + block, j * LANES : (j + 1) * LANES]
                    deep = column_ref[2, row : row + block, :] - source[j][2]
                    if t < LANES:
                        squared = deep * deep + known
                    else:
                        sep = [column_ref[k, row : row + block, :] - source[j][k] for k in range(2)]
                        squared = sep[0] * sep[0] + sep[1] * sep[1] + (deep * deep + sigma_sq)
                    inverse = lax.rsqrt(squared)
                    square = inverse * inverse
                    kernel = square * inverse
                    values[u].append(kernel)
                    if t >= LANES:
                        values[1].append((kernel * square) * known)
            sum_ref[t // LANES] = sum_ref[t // LANES] + product(values[0], values[1], feature)

    def step(index, _):
        for j in range(unroll):
            one(index * unroll + j, j % 2)
        return 0

    ahead(0, 0)
    lax.fori_loop(0, steps // unroll, step, 0)

    def combined(index):
        part = slice(index % 2 * LANES, (index % 2 + 1) * LANES)
        parts = sum_ref[index // 2, 0:8, part] + sum_ref[index // 2, 8:16, part] + sum_ref[index // 2, 16:24, part]
        return parts + pltpu.roll(parts, block, 1)

    lane = lax.broadcasted_iota(jnp.int32, (8, LANES), 1)
    found = jnp.where(lane < block, combined(0), combined(1))
    near = combined(2)
    pulled = combined(3)

    def crossed(place, rows):
        return [
            place[1] * rows[2:3] - place[2] * rows[1:2] - rows[3:4],
            place[2] * rows[0:1] - place[0] * rows[2:3] - rows[4:5],
            place[0] * rows[1:2] - place[1] * rows[0:1] - rows[5:6],
        ]

    own = own_ref[0:GROUPS, :]
    slots = target_rows(own)
    alive = own_ref[GROUPS : GROUPS + 1, :]
    blob_place = [own[k : k + 1] - centre[k] for k in range(3)]
    slot_place = [slots[k] - centre[k] for k in range(3)]
    a = slots[3:]
    first = [
        a[1] * near[2:3] - a[2] * near[1:2],
        a[2] * near[0:1] - a[0] * near[2:3],
        a[0] * near[1:2] - a[1] * near[0:1],
    ]
    blob_velocity = crossed(blob_place, found)
    slot_velocity = crossed(slot_place, near)
    second = crossed(slot_place, pulled)
    for k in range(3):
        blob_ref[k : k + 1, :] = -kernel_scale * blob_velocity[k]
        rates_ref[k : k + 1, :] = (-kernel_scale * slot_velocity[k] * alive)[:, 0:half]
        rates_ref[3 + k : 4 + k, :] = (-kernel_scale * (first[k] - 3.0 * second[k]) * alive)[:, 0:half]


def partners(count, start):
    pairs = [(i, i + 1) for i in range(start, count - 1, 2)]
    return pairs + [(j, i) for i, j in pairs]


def per_device(positions, strengths, live_counts, vorticity, diffusivity, seed_counts):
    _, cells_x, cells_y, cells_z = vorticity.shape
    slot_count = positions.shape[1]
    y_axes = ("src", "grp")
    everyone = ("tgt", "src", "grp")
    x_count, y_count = lax.axis_size("tgt"), lax.axis_size("src") * lax.axis_size("grp")
    devices = x_count * y_count
    f32 = jnp.float32

    def kept(*shape):
        return pltpu.VMEM(shape, f32)

    def held(array):
        return pltpu.with_memory_space_constraint(array, pltpu.VMEM)

    def number(x, y):
        return x * y_count + y

    second, third = [], []
    for y in range(y_count):
        crossed, straight = (second, third) if (y + 1) // 2 % 2 == 1 else (third, second)
        straight += [(number(i, y), number(j, y)) for i, j in partners(x_count, 0)]
        crossed += [(number(x, i), number(x, j)) for i, j in partners(y_count, 1) for x in range(x_count) if i == y]
    tall = max(cells_x, cells_y)
    xb, ya, two, three = pl.pallas_call(
        faces_kernel,
        name="faces",
        out_shape=(kept(3, cells_y, cells_z), kept(3, cells_x, cells_z), kept(3, tall, cells_z), kept(3, tall, cells_z)),
        in_specs=[pl.BlockSpec(memory_space=pl.ANY)],
        out_specs=[VMEM] * 4,
        scratch_shapes=[
            pltpu.VMEM((3, cells_y, cells_z), f32),
            pltpu.VMEM((3, cells_x, 1, cells_z), f32),
            pltpu.VMEM((3, cells_x, 1, cells_z), f32),
            pltpu.SemaphoreType.DMA((4,)),
        ],
    )(vorticity)
    xb = held(lax.ppermute(xb, "tgt", partners(x_count, 1)))
    two = held(lax.ppermute(two, everyone, second))
    three = held(lax.ppermute(three, everyone, third))
    ya = held(lax.ppermute(ya, y_axes, partners(y_count, 0)))

    v, d, c = vorticity, diffusivity, seed_counts
    sums, wx, wy, rows = pl.pallas_call(
        local_kernel,
        name="local",
        out_shape=(kept(8, cells_z), kept(2, cells_y, cells_z), kept(2, cells_x, cells_z), kept(8, LANES)),
        in_specs=[VMEM] * 6,
        out_specs=[VMEM] * 4,
    )(live_counts.reshape(1, 1), v, d, c, positions, strengths)
    block, own = pl.pallas_call(
        block_kernel,
        name="block",
        out_shape=(jax.ShapeDtypeStruct((devices * GROUPS, LANES), f32), kept(16, LANES)),
        in_specs=[VMEM] * 8,
        out_specs=[VMEM] * 2,
    )(held(sums), held(wx), held(wy), held(rows), xb, ya, two, three)
    everything = lax.all_to_all(block.reshape(-1), everyone, 0, 0, tiled=True).reshape(devices * GROUPS, LANES)

    targets = LANES + slot_count
    vorticity_next, columns, factors = pl.pallas_call(
        grid_kernel,
        name="grid",
        out_shape=(jax.ShapeDtypeStruct(vorticity.shape, f32), kept(3, targets, LANES), pltpu.VMEM((targets, LANES), jnp.bfloat16)),
        in_specs=[VMEM] * 7,
        out_specs=[VMEM] * 3,
    )(vorticity, diffusivity, xb, ya, two, three, held(own))

    tiles = devices + devices // 2
    pitch = tiles + 1 - tiles % 2
    particle_rates, blob_velocity = pl.pallas_call(
        functools.partial(pair_kernel, cells=(cells_x, cells_y, cells_z)),
        name="pairs",
        out_shape=(jax.ShapeDtypeStruct((6, slot_count), f32), jax.ShapeDtypeStruct((3, LANES), f32)),
        in_specs=[VMEM] * 4,
        out_specs=[VMEM, VMEM],
        scratch_shapes=[
            pltpu.VMEM((3 * tiles, LANES), f32),
            pltpu.VMEM((16 * pitch, LANES), f32),
            pltpu.VMEM((32 * pitch, LANES), f32),
            pltpu.VMEM((devices, LANES), f32),
            pltpu.VMEM((2, targets, 4 * LANES), f32),
            pltpu.VMEM((2, 32, 2 * LANES), f32),
        ],
    )(held(everything), held(own), held(columns), held(factors))
    return (vorticity_next, particle_rates, blob_velocity)


def solution(mesh):
    placed = (
        P(None, ("tgt", "src", "grp")),
        P(None, ("tgt", "src", "grp")),
        P(("tgt", "src", "grp")),
        P(None, "tgt", ("src", "grp"), None),
        P("tgt", ("src", "grp"), None),
        P("tgt", ("src", "grp"), None),
    )
    return jax.shard_map(
        per_device,
        mesh=mesh,
        in_specs=placed,
        out_specs=(
            P(None, "tgt", ("src", "grp"), None),
            P(None, ("tgt", "src", "grp")),
            P(None, ("tgt", "src", "grp")),
        ),
        check_vma=False,
    )
```
